128 devices in a mesh: stream: 16 (over x, z), cy: 4 (over y), cz: 2 (over core).
Axes of the slice: x: 4, y: 4, z: 4, core: 2. Of those that a mesh axis runs over, the one named last changes fastest.
Arguments:
- populations: float32 [1536, 19, 4096], P(('stream', 'cy', 'cz')), may hold values from 0.2 to 1
- solid_cells: int32 [1536, 4096], P(('stream', 'cy', 'cz')), may hold values 0 or 1
- block_pos: int32 [1536, 3], P(('stream', 'cy', 'cz')), may hold values from -1 to 31, as said below
Outputs:
- populations_out: float32 [19, 512, 64, 128], P(None, 'stream', 'cy', 'cz')
The draws below stay inside these ranges and needn't reach their ends.
Inputs may be any that keep to these rules, and one draw needn't show every extreme that they name: `block_pos`: row r belongs to device r // 12 in mesh order. A device's rows hold, in order, a run of its (cy, cz) group's block list followed by rows of -1. The list names once every block with by in the group's 1 block and bz in its 4 blocks, ordered by bx, blocks of one bx in any order. The device at index s of stream holds the entries from s * 8 + d_s up to (s + 1) * 8 + d_(s+1), where d is 0 at both ends of the axis and |d_s| <= 2; so its rows name at most 2 blocks with bx // 2 equal to each of s - 1 and s + 1, no other foreign ones, and at most 4 of its own blocks lie on other devices.
All inputs are finite; a program needn't handle non-finite values. No bound on the sum of `solid_cells` on one device may be relied on, other than what follows from the above.
Results may differ from the reference program's by a relative error of at most 0.0001.
Values sent between devices are 32-bit elements; how exact they have to be, the bound alone decides.
A program may use at most 128 MiB of HBM per device.

```python
import jax
import jax.numpy as jnp

EDGE = 16
BXD = 2
BYD = 1
BZD = 4
STEPS = 2
MOVE_CAP = 2
SLOTS = 8
OLD_SLOTS = 12
ROWS = 1536
NXC = 512
NYC = 64
NZC = 128
N_STREAM = 16
N_CY = 4
N_CZ = 2


def draw_block_pos(key, part):
    groups = N_CY * N_CZ
    per_layer = BYD * BZD
    layers = BXD * N_STREAM
    key_delta = jax.random.fold_in(key, 11)
    key_spot = jax.random.fold_in(key, 12)
    key_order = jax.random.fold_in(key, 13)
    offsets = jax.random.randint(key_delta, (groups, N_STREAM + 1), -MOVE_CAP, MOVE_CAP + 1)
    column = jnp.arange(N_STREAM + 1)[None, :]
    spot = jax.random.randint(key_spot, (groups, 1), 1, N_STREAM - 2)
    offsets = jnp.where(column == spot, MOVE_CAP, offsets)
    offsets = jnp.where(column == spot + 1, -MOVE_CAP, offsets)
    offsets = jnp.where(column == spot + 2, MOVE_CAP, offsets)
    offsets = jnp.where((column == 0) | (column == N_STREAM), 0, offsets)
    cuts = column * SLOTS + offsets
    starts = cuts[:, :-1]
    counts = cuts[:, 1:] - cuts[:, :-1]
    slot_index = jnp.arange(OLD_SLOTS)
    entry = starts[:, :, None] + slot_index[None, None, :]
    occupied = slot_index[None, None, :] < counts[:, :, None]
    entry = jnp.where(occupied, entry, 0)
    scores = jax.random.randint(key_order, (groups, layers, per_layer), 0, 1 << 20) * per_layer
    scores = scores + jnp.arange(per_layer)[None, None, :]
    ordering = jnp.argsort(scores, axis=-1)
    layer = entry // per_layer
    within = entry % per_layer
    group_index = jnp.arange(groups)[:, None, None]
    placed = ordering[group_index, layer, within]
    group_y = group_index // N_CZ
    group_z = group_index % N_CZ
    coord_x = layer
    coord_y = group_y * BYD + placed // BZD
    coord_z = group_z * BZD + placed % BZD
    coords = jnp.stack([coord_x, coord_y, coord_z], axis=-1)
    coords = jnp.where(occupied[..., None], coords, -1)
    coords = jnp.transpose(coords, (1, 0, 2, 3))
    return coords.reshape(N_STREAM * groups * OLD_SLOTS, 3).astype(jnp.int32)


def with_ends(array, stream_key, low, high):
    index_at = [jax.random.randint(jax.random.fold_in(stream_key, axis), (), 0, length) for axis, length in enumerate(array.shape)]
    widest = array.shape.index(max(array.shape))
    beside = index_at[:widest] + [(index_at[widest] + 1) % array.shape[widest]] + index_at[widest + 1:]
    return array.at[tuple(index_at)].set(low).at[tuple(beside)].set(high)


def shard_levels(own_key, shape, cuts, least, top_value):
    factor_of = 1.0
    for position, shards_of in cuts:
        draws = jax.random.uniform(jax.random.fold_in(jax.random.fold_in(own_key, 6), position), (shards_of,), jnp.float32, least / len(cuts), top_value / len(cuts))
        factor_of = factor_of * jnp.repeat(jnp.exp(draws), shape[position] // shards_of).reshape((-1,) + (1,) * (len(shape) - 1 - position))
    return factor_of


def setup_inputs(seed: int = 0) -> dict:
    key_list = jax.random.split(jax.random.key(seed), 4)
    return {
        "populations": jnp.clip(0.2 + 0.8 * jax.random.uniform(key_list[0], (ROWS, 19, EDGE**3), jnp.float32) ** shard_levels(key_list[0], (ROWS, 19, EDGE**3), ((0, 128),), -0.2, 0.2), 0.2, 1.0),
        "solid_cells": with_ends((jax.random.randint(key_list[1], (ROWS, EDGE**3), 0, 8) < 1).astype(jnp.int32), jax.random.fold_in(key_list[1], 1), 0, 1),
        "block_pos": draw_block_pos(jax.random.fold_in(key_list[3], 71), 0),
    }


VELOCITIES = ((0, 0, 0), (1, 0, 0), (-1, 0, 0), (0, 1, 0), (0, -1, 0), (0, 0, 1), (0, 0, -1),
              (1, 1, 0), (-1, -1, 0), (1, -1, 0), (-1, 1, 0), (1, 0, 1), (-1, 0, -1),
              (1, 0, -1), (-1, 0, 1), (0, 1, 1), (0, -1, -1), (0, 1, -1), (0, -1, 1))
WEIGHTS = (1.0 / 3.0,) + (1.0 / 18.0,) * 6 + (1.0 / 36.0,) * 12
OPPOSITE = (0, 2, 1, 4, 3, 6, 5, 8, 7, 10, 9, 12, 11, 14, 13, 16, 15, 18, 17)
OMEGA_EVEN = 1.25
OMEGA_ODD = 1.0 / 1.125


def moment(lattice, component):
    summed = jnp.zeros_like(lattice[0])
    for member in range(19):
        factor = VELOCITIES[member][component]
        if factor == 1:
            summed = summed + lattice[member]
        elif factor == -1:
            summed = summed - lattice[member]
    return summed


def collide(lattice):
    density = jnp.sum(lattice, axis=0)
    velocity = [moment(lattice, component) / density for component in range(3)]
    square = velocity[0] * velocity[0] + velocity[1] * velocity[1] + velocity[2] * velocity[2]
    outputs = []
    for member in range(19):
        step_x, step_y, step_z = VELOCITIES[member]
        projected = step_x * velocity[0] + step_y * velocity[1] + step_z * velocity[2]
        even_eq = WEIGHTS[member] * density * (1.0 + 4.5 * projected * projected - 1.5 * square)
        odd_eq = WEIGHTS[member] * density * 3.0 * projected
        mirror = lattice[OPPOSITE[member]]
        even_part = 0.5 * (lattice[member] + mirror)
        odd_part = 0.5 * (lattice[member] - mirror)
        outputs.append(lattice[member] - OMEGA_EVEN * (even_part - even_eq) - OMEGA_ODD * (odd_part - odd_eq))
    return jnp.stack(outputs), density


def propagate(lattice, widened, wall_ext, drift_y, drift_z, density, rotor_here):
    size_x, size_y, size_z = lattice.shape[1:]
    outputs = []
    for member in range(19):
        step_x, step_y, step_z = VELOCITIES[member]
        window = (slice(1 - step_x, 1 - step_x + size_x), slice(1 - step_y, 1 - step_y + size_y),
                  slice(1 - step_z, 1 - step_z + size_z))
        pulled = widened[member][window]
        blocked = wall_ext[window]
        wall_push = 6.0 * WEIGHTS[member] * density * (step_y * drift_y[window] + step_z * drift_z[window])
        bounced = widened[OPPOSITE[member]][1:1 + size_x, 1:1 + size_y, 1:1 + size_z] + wall_push
        read = jnp.where(blocked, bounced, pulled)
        outputs.append(jnp.where(rotor_here, lattice[member], read))
    return jnp.stack(outputs)


def reference(populations, solid_cells, block_pos):
    block_cells = EDGE ** 3
    count_x = BXD * N_STREAM
    count_y = BYD * N_CY
    count_z = BZD * N_CZ
    blocks_all = count_x * count_y * count_z
    occupied = block_pos[:, 0] >= 0
    ident = (block_pos[:, 0] * count_y + block_pos[:, 1]) * count_z + block_pos[:, 2]
    ident = jnp.where(occupied, ident, blocks_all).astype(jnp.int32)
    placed = jnp.zeros((blocks_all + 1, 19, block_cells), jnp.float32).at[ident].set(populations)[:blocks_all]
    lattice = placed.reshape(count_x, count_y, count_z, 19, EDGE, EDGE, EDGE)
    lattice = lattice.transpose(3, 0, 4, 1, 5, 2, 6).reshape(19, NXC, NYC, NZC)
    placed_marks = jnp.zeros((blocks_all + 1, block_cells), jnp.int32).at[ident].set(solid_cells)[:blocks_all]
    marks = placed_marks.reshape(count_x, count_y, count_z, EDGE, EDGE, EDGE)
    marks = marks.transpose(0, 3, 1, 4, 2, 5).reshape(NXC, NYC, NZC)
    rotor_here = marks == 1
    wall_ext = jnp.pad(rotor_here, 1, constant_values=True)
    rotor_ext = jnp.pad(rotor_here, 1, constant_values=False)
    spin = 0.2 / (NYC + NZC)
    centre_y = (NYC - 1) / 2.0
    centre_z = (NZC - 1) / 2.0
    coord_y = (jnp.arange(NYC + 2) - 1).astype(jnp.float32)
    coord_z = (jnp.arange(NZC + 2) - 1).astype(jnp.float32)
    drift_y = jnp.where(rotor_ext, -spin * (coord_z - centre_z)[None, None, :], 0.0)
    drift_z = jnp.where(rotor_ext, spin * (coord_y - centre_y)[None, :, None], 0.0)
    for sweep in range(STEPS):
        post, density = collide(lattice)
        widened = jnp.pad(post, ((0, 0), (1, 1), (1, 1), (1, 1)))
        lattice = propagate(lattice, widened, wall_ext, drift_y, drift_z, density, rotor_here)
    return lattice
```

```python
import jax
import jax.numpy as jnp
from jax import lax
from jax.experimental import pallas as pl
from jax.experimental.pallas import tpu as pltpu
from jax.sharding import PartitionSpec as P

MESH = pl.DeviceIdType.MESH
F32 = jnp.float32

GROUPS = (
    (0, 0, 0, 5, 6),
    (1, 0, 1, 11, 13),
    (-1, 0, 2, 14, 12),
    (0, 1, 3, 15, 17),
    (0, -1, 4, 18, 16),
)
DIAGONALS = ((1, 1, 7), (-1, -1, 8), (1, -1, 9), (-1, 1, 10))
PAIRS = ((1, 2), (3, 4), (5, 6), (7, 8), (9, 10), (11, 12), (13, 14), (15, 16), (17, 18))
OPPOSITE = (0, 2, 1, 4, 3, 6, 5, 8, 7, 10, 9, 12, 11, 14, 13, 16, 15, 18, 17)
UP_X = (1, 7, 9, 11, 13)
DOWN_X = (2, 8, 10, 12, 14)
UP_Y = (3, 7, 10, 15, 17)
DOWN_Y = (4, 8, 9, 16, 18)
MARK = 19

EDGE = 16
CHUNKS = 4
PLANES = EDGE // CHUNKS
TILES = 2 * PLANES
ROWS = 12
OMEGA = 0.2 / 192.0


def roll(value, shift, axis=1):
    return pltpu.roll(value, shift % value.shape[axis] if isinstance(shift, int) else shift, axis)


def collide(f, mark):
    plus = [f[i] + f[o] for i, o in PAIRS]
    minus = [f[i] - f[o] for i, o in PAIRS]
    density = f[0] + ((plus[0] + plus[1]) + (plus[2] + plus[3])) + (
        (plus[4] + plus[5]) + (plus[6] + plus[7]) + plus[8]
    )
    mx = (minus[0] + minus[3]) + (minus[4] + minus[5]) + minus[6]
    my = (minus[1] + minus[3]) - (minus[4] - minus[7]) + minus[8]
    mz = (minus[2] + minus[5]) - (minus[6] - minus[7]) - minus[8]
    inverse = 1.0 / density
    base = density - 1.5 * (mx * mx + my * my + mz * mz) * inverse
    squared = 4.5 * inverse
    along = (mx, my, mz, mx + my, mx - my, mx + mz, mx - mz, my + mz, my - mz)
    post = [None] * 19
    post[0] = f[0] - 1.25 * (f[0] - (1.0 / 3.0) * base)
    for k, (i, o) in enumerate(PAIRS):
        weight = 1.0 / 18.0 if k < 3 else 1.0 / 36.0
        m = along[k]
        even = 0.625 * plus[k] - (1.25 * weight) * (base + squared * (m * m))
        odd = (4.0 / 9.0) * minus[k] - (8.0 / 3.0 * weight) * m
        post[i] = f[i] - even - odd
        post[o] = f[o] - even + odd
    return [jnp.where(mark, f[i], post[i]) for i in range(19)], density


def group_swap(values):
    lane = lax.broadcasted_iota(jnp.int32, values[0].shape, 1)
    for bit in range(3):
        step = 1 << bit
        high = (lane // (16 * step)) % 2 == 1
        out = list(values)
        for i in range(8):
            if i & step:
                continue
            low_one, high_one = values[i], values[i + step]
            out[i] = jnp.where(high, roll(high_one, 16 * step), low_one)
            out[i + step] = jnp.where(high, high_one, roll(low_one, -16 * step))
        values = out
    return values


def kernel(pos, held, mark_in, out, held_marks, send, recv, stage, ext1, ext2, rho, walls,
           rotors, face_x, face_y, face_z, edge_xy, edge_yz, edge_xz,
           got_x, got_y, got_z, got_xy, got_yz, got_xz, zext,
           move_send, move_recv, halo_send, halo_recv):
    s = lax.axis_index("stream")
    cy = lax.axis_index("cy")
    core = lax.axis_index("cz")
    n_s = lax.axis_size("stream")
    n_y = lax.axis_size("cy")
    up_s, down_s = lax.rem(s + 1, n_s), lax.rem(s + n_s - 1, n_s)
    up_y, down_y = lax.rem(cy + 1, n_y), lax.rem(cy + n_y - 1, n_y)
    other = 1 - core
    partners = (
        (up_s, cy, core), (down_s, cy, core), (s, up_y, core), (s, down_y, core), (s, cy, other),
        (up_s, up_y, core), (down_s, down_y, core), (up_s, down_y, core), (down_s, up_y, core),
        (s, up_y, other), (s, down_y, other), (up_s, cy, other), (down_s, cy, other),
    )

    barrier = pltpu.get_barrier_semaphore()
    for partner in partners:
        pl.semaphore_signal(barrier, inc=1, device_id=partner, device_id_type=MESH)

    source = [jnp.int32(-1)] * 8
    up_row = [jnp.int32(0), jnp.int32(0)]
    down_row = [jnp.int32(0), jnp.int32(0)]
    up_low, up_high = jnp.int32(99), jnp.int32(-1)
    down_low, down_high = jnp.int32(99), jnp.int32(-1)
    for r in range(ROWS):
        bx = pos[0, r]
        layer = bx - 2 * s
        bz = pos[2, r] - 4 * core
        spot = jnp.where((layer >= 0) & (layer < 2) & (bx >= 0), layer * 4 + bz, -1)
        source = [jnp.where(spot == j, r, source[j]) for j in range(8)]
        rises = layer >= 2
        sinks = (layer < 0) & (bx >= 0)
        less, more = rises & (bz < up_low), rises & (bz > up_high)
        up_row = [jnp.where(less, r, up_row[0]), jnp.where(more, r, up_row[1])]
        up_low, up_high = jnp.where(less, bz, up_low), jnp.where(more, bz, up_high)
        less, more = sinks & (bz < down_low), sinks & (bz > down_high)
        down_row = [jnp.where(less, r, down_row[0]), jnp.where(more, r, down_row[1])]
        down_low, down_high = jnp.where(less, bz, down_low), jnp.where(more, bz, down_high)
    order = []
    for layer in range(2):
        missing = jnp.int32(0)
        for z in range(4):
            order.append(jnp.minimum(missing, 1))
            missing = missing + jnp.where(source[layer * 4 + z] < 0, 1, 0)
    here = [jnp.full((8, 128), source[j], jnp.int32) >= 0 for j in range(8)]
    here4 = [jnp.full((4, 128), source[j], jnp.int32) >= 0 for j in range(8)]
    later = [jnp.full((8, 128), order[j], jnp.int32) > 0 for j in range(8)]
    second = [jnp.full((4, 128), order[j], jnp.int32) > 0 for j in range(8)]
    source = [jnp.maximum(source[j], 0) for j in range(8)]

    for r in range(ROWS):
        held_marks[r] = mark_in[r:r + 1, :].astype(F32)

    def cells(k):
        return pl.ds(pl.multiple_of(k * 128, 128), 128)

    def tail(row, k):
        marks = held_marks[row, :, cells(k)]
        return jnp.concatenate([held[row, 16:19, cells(k)], marks], axis=0)

    def move(d, c):
        return pltpu.make_async_remote_copy(
            src_ref=send.at[d, c], dst_ref=recv.at[d, c],
            send_sem=move_send.at[d, c], recv_sem=move_recv.at[d, c],
            device_id=partners[d], device_id_type=MESH,
        )

    def pack(c):
        @pl.loop(0, TILES)
        def _(kk):
            k = c * TILES + kk
            for d, rows in ((0, up_row), (1, down_row)):
                for q in range(2):
                    send[d, c, kk, 2 * q] = held[rows[q], 0:8, cells(k)]
                    send[d, c, kk, 2 * q + 1] = held[rows[q], 8:16, cells(k)]
                send[d, c, kk, 4] = jnp.concatenate(
                    [tail(rows[0], k), tail(rows[1], k)], axis=0)

    for c in range(CHUNKS):
        pack(c)
        if c == 0:
            pl.semaphore_wait(barrier, len(partners))
        move(0, c).start()
        move(1, c).start()

    lane = lax.broadcasted_iota(jnp.int32, (8, 128), 1)
    low_half = lane < 64

    def settle(c, carry):
        move(0, c).wait_recv()
        move(1, c).wait_recv()

        @pl.loop(0, PLANES)
        def _(plane):
            a = c * PLANES + plane
            for h in range(2):
                kk = plane * 2 + h
                k = c * TILES + kk
                for t in range(3):
                    tiles = []
                    for j in range(8):
                        d = j // 4
                        if t < 2:
                            mine = held[source[j], 8 * t:8 * t + 8, cells(k)]
                            theirs = jnp.where(later[j], recv[d, c, kk, 2 + t], recv[d, c, kk, t])
                            tiles.append(jnp.where(here[j], mine, theirs))
                        else:
                            theirs = recv[d, c, kk, 4]
                            theirs = jnp.where(second[j], theirs[4:8], theirs[0:4])
                            tiles.append(jnp.where(here4[j], tail(source[j], k), theirs))
                    height = tiles[0].shape[0]
                    for g, value in enumerate(group_swap(tiles)):
                        stage[t, 8 * g:8 * g + height, :] = value
                f = [stage[p // 8, pl.ds(p % 8, 8, stride=8), :] for p in range(19)]
                marks = stage[2, pl.ds(3, 8, stride=8), :]
                post, density = collide(f, marks > 0.5)
                for p in range(19):
                    ext1[p, a + 1, 8 + 8 * h:16 + 8 * h, :] = post[p]
                ext1[MARK, a + 1, 8 + 8 * h:16 + 8 * h, :] = marks
                rho[a, 8 * h:8 * h + 8, :] = density
        return carry

    lax.fori_loop(0, CHUNKS, settle, 0)

    z_edge = jnp.where(core == 0, 63, 0)
    sent_z = [jnp.where(core == 0, group[3], group[4]) for group in GROUPS] + [MARK]
    flat_lane = lane % 64

    def messages(step):
        n = 6 if step == 0 else 5
        refs = []
        for d in range(2):
            refs.append((face_x.at[step, d, pl.ds(0, n)], got_x.at[step, d, pl.ds(0, n)]))
        for d in range(2):
            refs.append((face_y.at[step, d, pl.ds(0, n)], got_y.at[step, d, pl.ds(0, n)]))
        refs.append((face_z.at[step, pl.ds(0, n)], got_z.at[step, pl.ds(0, n)]))
        for e in range(4):
            refs.append((edge_xy.at[step, e], got_xy.at[step, e]))
        for e in range(2):
            refs.append((edge_yz.at[step, e], got_yz.at[step, e]))
        for e in range(2):
            refs.append((edge_xz.at[step, e], got_xz.at[step, e]))
        return [
            pltpu.make_async_remote_copy(
                src_ref=src, dst_ref=dst, send_sem=halo_send.at[step, i],
                recv_sem=halo_recv.at[step, i], device_id=partners[i], device_id_type=MESH,
            )
            for i, (src, dst) in enumerate(refs)
        ]

    def exchange(ext, step):
        n = 6 if step == 0 else 5
        flat = ext.reshape(20, 18 * 32, 128)
        for d, pops in ((0, UP_X), (1, DOWN_X)):
            plane = 16 if d == 0 else 1
            for j, p in enumerate((pops + (MARK,))[:n]):
                for h in range(2):
                    face_x[step, d, j, 8 * h:8 * h + 8, :] = roll(
                        ext[p, plane, 8 + 8 * h:16 + 8 * h, :], 64)
        for d, pops in ((0, UP_Y), (1, DOWN_Y)):
            row = 23 if d == 0 else 8
            for j, p in enumerate((pops + (MARK,))[:n]):
                for h in range(2):
                    face_y[step, d, j, 8 * h:8 * h + 8, :] = flat[
                        p, pl.ds(32 * (1 + 8 * h) + row, 8, stride=32), :]

        def gather(a, totals):
            shift = lax.rem(a + 1 - z_edge + 128, 128)
            keep = flat_lane == a + 1
            return tuple(
                jnp.where(keep, roll(ext[sent_z[j], a + 1, 8 + 8 * h:16 + 8 * h, :], shift),
                          totals[2 * j + h])
                for j in range(n) for h in range(2)
            )

        zero = jnp.zeros((8, 128), F32)
        totals = lax.fori_loop(0, EDGE, gather, (zero,) * (2 * n))
        for j in range(n):
            for h in range(2):
                face_z[step, j, 8 * h:8 * h + 8, :] = totals[2 * j + h]
        for e, (d, j, row) in enumerate(((0, 1, 15), (1, 1, 0), (0, 2, 0), (1, 2, 15))):
            edge_xy[step, e, 0:1, :] = face_x[step, d, j, row:row + 1, :]
            if step == 0:
                edge_xy[step, e, 1:2, :] = face_x[step, d, 5, row:row + 1, :]
        for e, (j, row) in enumerate(((3, 15), (4, 0))):
            edge_yz[step, e, 0:1, :] = face_z[step, j, row:row + 1, :]
            if step == 0:
                edge_yz[step, e, 1:2, :] = face_z[step, 5, row:row + 1, :]
        for e, j in enumerate((1, 2)):
            for h in range(2):
                value = totals[2 * j + h]
                if step == 0:
                    at = 80 if e == 0 else 1
                    value = jnp.where(lane == at, value, roll(totals[10 + h], 1))
                edge_xz[step, e, 8 * h:8 * h + 8, :] = value

        copies = messages(step)
        for copy in copies:
            copy.start()
        for copy in copies:
            copy.wait_recv()

        for d, pops, row in ((0, UP_Y, 7), (1, DOWN_Y, 24)):
            outside = (cy == 0) if d == 0 else (cy == n_y - 1)
            for j, p in enumerate((pops + (MARK,))[:n]):
                for h in range(2):
                    value = got_y[step, d, j, 8 * h:8 * h + 8, :]
                    if p == MARK:
                        value = jnp.where(outside, jnp.full_like(value, 2.0), value)
                    flat[p, pl.ds(32 * (1 + 8 * h) + row, 8, stride=32), :] = value
        for d, pops in ((0, UP_X), (1, DOWN_X)):
            plane, behind = (0, 16) if d == 0 else (17, 1)
            beyond = low_half if d == 0 else jnp.logical_not(low_half)
            outside = (s == 0) if d == 0 else (s == n_s - 1)
            for j, p in enumerate((pops + (MARK,))[:n]):
                for h in range(2):
                    value = got_x[step, d, j, 8 * h:8 * h + 8, :]
                    if p == MARK:
                        value = jnp.where(outside, jnp.full_like(value, 2.0), value)
                    ext[p, plane, 8 + 8 * h:16 + 8 * h, :] = jnp.where(
                        beyond, value, face_x[step, d, j, 8 * h:8 * h + 8, :])
        for e, (d, p, row) in enumerate(((0, 7, 7), (1, 8, 24), (0, 9, 24), (1, 10, 7))):
            plane, behind = (0, 16) if d == 0 else (17, 1)
            beyond = (low_half if d == 0 else jnp.logical_not(low_half))[0:1]
            own = roll(ext[p, behind, row:row + 1, :], 64)
            ext[p, plane, row:row + 1, :] = jnp.where(beyond, got_xy[step, e, 0:1, :], own)
            if step == 0:
                out_x = (s == 0) if d == 0 else (s == n_s - 1)
                out_y = (cy == 0) if row == 7 else (cy == n_y - 1)
                value = got_xy[step, e, 1:2, :]
                value = jnp.where(out_x | out_y, jnp.full_like(value, 2.0), value)
                own = roll(ext[MARK, behind, row:row + 1, :], 64)
                ext[MARK, plane, row:row + 1, :] = jnp.where(beyond, value, own)
        for j in range(n):
            low_side = j in (1, 5)
            high_side = j in (2, 5)
            for h in range(2):
                value = got_z[step, j, 8 * h:8 * h + 8, :]
                fixed = value
                if low_side:
                    far = roll(got_xz[step, 0, 8 * h:8 * h + 8, :], 128 - (80 if j == 1 else 81))
                    if j == 5:
                        far = jnp.where(s == 0, jnp.full_like(far, 2.0), far)
                    fixed = jnp.where(lane == 64, roll(value, 48), fixed)
                    fixed = jnp.where(lane == 0, far, fixed)
                if high_side:
                    far = roll(got_xz[step, 1, 8 * h:8 * h + 8, :], 80 if j == 2 else 79)
                    if j == 5:
                        far = jnp.where(s == n_s - 1, jnp.full_like(far, 2.0), far)
                    fixed = jnp.where(lane == 17, roll(value, 80), fixed)
                    fixed = jnp.where(lane == 81, far, fixed)
                zext[step, j, 8 + 8 * h:16 + 8 * h, :] = fixed
        zext[step, 3, 7:8, :] = got_yz[step, 0, 0:1, :]
        zext[step, 4, 24:25, :] = got_yz[step, 1, 0:1, :]
        if step == 0:
            for e, row in ((0, 7), (1, 24)):
                outside = (cy == 0) if e == 0 else (cy == n_y - 1)
                value = got_yz[step, e, 1:2, :]
                zext[step, 5, row:row + 1, :] = jnp.where(
                    outside, jnp.full_like(value, 2.0), value)
        for copy in copies:
            copy.wait_send()

    first_z = flat_lane == 0
    last_z = flat_lane == 63
    z_target = jnp.where(core == 1, 0, 63)

    def rows(h, step_y):
        start = 8 + 8 * h - step_y
        return slice(start, start + 8)

    def z_halo(step, j, a, h, step_x, step_y):
        shift = lax.rem(z_target - a + (127 + step_x), 128)
        return roll(zext[step, j, rows(h, step_y), :], shift)

    def make_bits(a, carry):
        for h in range(2):
            wall = jnp.zeros((8, 128), jnp.int32)
            rotor = jnp.zeros((8, 128), jnp.int32)

            def add(bit, value):
                nonlocal wall, rotor
                wall = wall + jnp.where(value > 0.5, 1 << bit, 0)
                if bit > 2:
                    rotor = rotor + jnp.where(value == 1.0, 1 << bit, 0)

            for step_x, step_y, p_flat, p_up, p_down in GROUPS:
                value = ext1[MARK, a + 1 - step_x, rows(h, step_y), :]
                add(p_flat, value)
                halo = z_halo(0, 5, a, h, step_x, step_y)
                add(p_up, jnp.where(
                    first_z, jnp.where(core == 1, halo, jnp.full_like(halo, 2.0)), roll(value, 1)))
                add(p_down, jnp.where(
                    last_z, jnp.where(core == 0, halo, jnp.full_like(halo, 2.0)), roll(value, -1)))
            for step_x, step_y, p in DIAGONALS:
                add(p, ext1[MARK, a + 1 - step_x, rows(h, step_y), :])
            walls[a, 8 * h:8 * h + 8, :] = wall
            rotors[a, 8 * h:8 * h + 8, :] = rotor
        return carry

    along_z = (core * 64 + flat_lane).astype(F32) - 63.5
    drift_a = (-OMEGA / 6.0) * along_z
    sub = lax.broadcasted_iota(jnp.int32, (8, 128), 0)

    def pull(ext, step, a, h):
        here_rows = slice(8 + 8 * h, 16 + 8 * h)
        centre = [ext[p, a + 1, here_rows, :] for p in range(19)]
        wall = walls[a, 8 * h:8 * h + 8, :]
        rotor = rotors[a, 8 * h:8 * h + 8, :]
        density = rho[a, 8 * h:8 * h + 8, :]
        along_y = (cy * 16 + 8 * h + sub).astype(F32) - 31.5
        push_a = density * drift_a
        push_b = density * ((OMEGA / 6.0) * along_y)
        both, apart = push_a + push_b, push_a - push_b
        push = {
            3: 2.0 * push_a, 4: -2.0 * push_a, 5: 2.0 * push_b, 6: -2.0 * push_b,
            7: push_a, 8: -push_a, 9: -push_a, 10: push_a,
            11: push_b, 12: -push_b, 13: -push_b, 14: push_b,
            15: both, 16: -both, 17: apart, 18: -apart,
        }
        solid = (wall & 1) != 0
        new = [None] * 19
        new[0] = centre[0]

        def settle_one(p, pulled):
            bounced = centre[OPPOSITE[p]]
            if p > 2:
                bounced = bounced + jnp.where((rotor & (1 << p)) != 0, push[p], 0.0)
            value = jnp.where((wall & (1 << p)) != 0, bounced, pulled)
            new[p] = jnp.where(solid, centre[p], value)

        for j, (step_x, step_y, p_flat, p_up, p_down) in enumerate(GROUPS):
            if p_flat:
                settle_one(p_flat, ext[p_flat, a + 1 - step_x, rows(h, step_y), :])
            halo = z_halo(step, j, a, h, step_x, step_y)
            value = ext[p_up, a + 1 - step_x, rows(h, step_y), :]
            settle_one(p_up, jnp.where(first_z, halo, roll(value, 1)))
            value = ext[p_down, a + 1 - step_x, rows(h, step_y), :]
            settle_one(p_down, jnp.where(last_z, halo, roll(value, -1)))
        for step_x, step_y, p in DIAGONALS:
            settle_one(p, ext[p, a + 1 - step_x, rows(h, step_y), :])
        return new, solid

    exchange(ext1, 0)
    lax.fori_loop(0, EDGE, make_bits, 0)

    def middle(a, carry):
        for h in range(2):
            new, solid = pull(ext1, 0, a, h)
            post, density = collide(new, solid)
            for p in range(19):
                ext2[p, a + 1, 8 + 8 * h:16 + 8 * h, :] = post[p]
            rho[a, 8 * h:8 * h + 8, :] = density
        return carry

    lax.fori_loop(0, EDGE, middle, 0)
    exchange(ext2, 1)

    def last(a, carry):
        for h in range(2):
            new, _ = pull(ext2, 1, a, h)
            for p in range(19):
                out[p, a, 8 * h:8 * h + 8, :] = new[p][:, 0:64]
                out[p, EDGE + a, 8 * h:8 * h + 8, :] = roll(new[p], 64)[:, 0:64]
        return carry

    lax.fori_loop(0, EDGE, last, 0)
    for c in range(CHUNKS):
        move(0, c).wait_send()
        move(1, c).wait_send()


def step_all(populations, solid_cells, block_pos):
    scratch = [
        pltpu.VMEM((ROWS, 1, 4096), F32),
        pltpu.VMEM((2, CHUNKS, TILES, 5, 8, 128), F32),
        pltpu.VMEM((2, CHUNKS, TILES, 5, 8, 128), F32),
        pltpu.VMEM((3, 64, 128), F32),
        pltpu.VMEM((20, 18, 32, 128), F32),
        pltpu.VMEM((20, 18, 32, 128), F32),
        pltpu.VMEM((EDGE, 16, 128), F32),
        pltpu.VMEM((EDGE, 16, 128), jnp.int32),
        pltpu.VMEM((EDGE, 16, 128), jnp.int32),
    ]
    for _ in range(2):
        scratch += [
            pltpu.VMEM((2, 2, 6, 16, 128), F32),
            pltpu.VMEM((2, 2, 6, 16, 128), F32),
            pltpu.VMEM((2, 6, 16, 128), F32),
            pltpu.VMEM((2, 4, 8, 128), F32),
            pltpu.VMEM((2, 2, 8, 128), F32),
            pltpu.VMEM((2, 2, 16, 128), F32),
        ]
    scratch += [
        pltpu.VMEM((2, 6, 32, 128), F32),
        pltpu.SemaphoreType.DMA((2, CHUNKS)),
        pltpu.SemaphoreType.DMA((2, CHUNKS)),
        pltpu.SemaphoreType.DMA((2, 13)),
        pltpu.SemaphoreType.DMA((2, 13)),
    ]
    return pl.pallas_call(
        kernel,
        out_shape=jax.ShapeDtypeStruct((19, 32, 16, 64), F32),
        in_specs=[
            pl.BlockSpec(memory_space=pltpu.SMEM),
            pl.BlockSpec(memory_space=pltpu.VMEM),
            pl.BlockSpec(memory_space=pltpu.VMEM),
        ],
        out_specs=pl.BlockSpec(memory_space=pltpu.VMEM),
        scratch_shapes=scratch,
        compiler_params=pltpu.CompilerParams(
            collective_id=0, has_side_effects=True, vmem_limit_bytes=40 * 1024 * 1024
        ),
    )(block_pos.T, populations, solid_cells)


def solution(mesh):
    in_specs = (
        P(("stream", "cy", "cz"), None, None),
        P(("stream", "cy", "cz"), None),
        P(("stream", "cy", "cz"), None),
    )
    out_specs = P(None, "stream", "cy", "cz")
    return jax.shard_map(step_all, mesh=mesh, in_specs=in_specs, out_specs=out_specs, check_vma=False)
```

```python
import jax
import jax.numpy as jnp
from jax import lax
from jax.experimental import pallas as pl
from jax.experimental.pallas import tpu as pltpu
from jax.sharding import PartitionSpec as P

MESH = pl.DeviceIdType.MESH
F32 = jnp.float32

GROUPS = (
    (0, 0, 0, 5, 6),
    (1, 0, 1, 11, 13),
    (-1, 0, 2, 14, 12),
    (0, 1, 3, 15, 17),
    (0, -1, 4, 18, 16),
)
DIAGONALS = ((1, 1, 7), (-1, -1, 8), (1, -1, 9), (-1, 1, 10))
PAIRS = ((1, 2), (3, 4), (5, 6), (7, 8), (9, 10), (11, 12), (13, 14), (15, 16), (17, 18))
OPPOSITE = (0, 2, 1, 4, 3, 6, 5, 8, 7, 10, 9, 12, 11, 14, 13, 16, 15, 18, 17)
UP_X = (1, 7, 9, 11, 13)
DOWN_X = (2, 8, 10, 12, 14)
UP_Y = (3, 7, 10, 15, 17)
DOWN_Y = (4, 8, 9, 16, 18)
MARK = 19

EDGE = 16
CHUNKS = 8
TILES = 4
OUTER = 7
ROWS = 12
OMEGA = 0.2 / 192.0
REVERSE = (1, 0, 3, 2, 4, 6, 5, 8, 7, 10, 9, 12, 11)


def roll(value, shift, axis=1):
    return pltpu.roll(value, shift % value.shape[axis] if isinstance(shift, int) else shift, axis)


def collide(f, mark):
    plus = [f[i] + f[o] for i, o in PAIRS]
    minus = [f[i] - f[o] for i, o in PAIRS]
    density = f[0] + ((plus[0] + plus[1]) + (plus[2] + plus[3])) + (
        (plus[4] + plus[5]) + (plus[6] + plus[7]) + plus[8]
    )
    mx = (minus[0] + minus[3]) + (minus[4] + minus[5]) + minus[6]
    my = (minus[1] + minus[3]) - (minus[4] - minus[7]) + minus[8]
    mz = (minus[2] + minus[5]) - (minus[6] - minus[7]) - minus[8]
    inverse = 1.0 / density
    base = density - 1.5 * (mx * mx + my * my + mz * mz) * inverse
    squared = 4.5 * inverse
    along = (mx, my, mz, mx + my, mx - my, mx + mz, mx - mz, my + mz, my - mz)
    post = [None] * 19
    post[0] = f[0] - 1.25 * (f[0] - (1.0 / 3.0) * base)
    for k, (i, o) in enumerate(PAIRS):
        weight = 1.0 / 18.0 if k < 3 else 1.0 / 36.0
        m = along[k]
        even = 0.625 * plus[k] - (1.25 * weight) * (base + squared * (m * m))
        odd = (4.0 / 9.0) * minus[k] - (8.0 / 3.0 * weight) * m
        post[i] = f[i] - even - odd
        post[o] = f[o] - even + odd
    return [jnp.where(mark, f[i], post[i]) for i in range(19)], density


def group_swap(values):
    lane = lax.broadcasted_iota(jnp.int32, values[0].shape, 1)
    for bit in range(3):
        step = 1 << bit
        high = (lane // (16 * step)) % 2 == 1
        out = list(values)
        for i in range(8):
            if i & step:
                continue
            low_one, high_one = values[i], values[i + step]
            out[i] = jnp.where(high, roll(high_one, 16 * step), low_one)
            out[i + step] = jnp.where(high, high_one, roll(low_one, -16 * step))
        values = out
    return values


def kernel(pos_in, pop_in, mark_in, out, held, marks_in, held_marks, pos, send, recv, stage, ext1, ext2,
           rho, walls, rotors, face_x, face_y, late_y, face_z, edge_xy, edge_yz, edge_xz,
           got_x, got_y, got_late_y, got_z, got_xy, got_yz, got_xz, zext,
           in_sem, move_send, move_recv, halo_send, halo_recv):
    s = lax.axis_index("stream")
    cy = lax.axis_index("cy")
    core = lax.axis_index("cz")
    n_s = lax.axis_size("stream")
    n_y = lax.axis_size("cy")
    up_s, down_s = lax.rem(s + 1, n_s), lax.rem(s + n_s - 1, n_s)
    up_y, down_y = lax.rem(cy + 1, n_y), lax.rem(cy + n_y - 1, n_y)
    other = 1 - core
    partners = (
        (up_s, cy, core), (down_s, cy, core), (s, up_y, core), (s, down_y, core), (s, cy, other),
        (up_s, up_y, core), (down_s, down_y, core), (up_s, down_y, core), (down_s, up_y, core),
        (s, up_y, other), (s, down_y, other), (up_s, cy, other), (down_s, cy, other),
    )
    above_s, below_s = s < n_s - 1, s > 0
    above_y, below_y = cy < n_y - 1, cy > 0
    exists = (
        above_s, below_s, above_y, below_y, None,
        above_s & above_y, below_s & below_y, above_s & below_y, below_s & above_y,
        above_y, below_y, above_s, below_s,
    )

    def when(condition, act):
        if condition is None:
            act()
        else:
            pl.when(condition)(act)

    loads = [pltpu.make_async_copy(pos_in, pos, in_sem.at[0]),
             pltpu.make_async_copy(mark_in, marks_in, in_sem.at[1])]
    loads += [
        pltpu.make_async_copy(pop_in.at[pl.ds(3 * i, 3)], held.at[pl.ds(3 * i, 3)], in_sem.at[2 + i])
        for i in range(4)
    ]
    for load in loads:
        load.start()
    barrier = pltpu.get_barrier_semaphore()
    arrivals = jnp.int32(0)
    for i, partner in enumerate(partners):
        when(exists[i], lambda partner=partner: pl.semaphore_signal(
            barrier, inc=1, device_id=partner, device_id_type=MESH))
        arrivals = arrivals + (1 if exists[i] is None else jnp.where(exists[i], 1, 0))

    loads[0].wait()
    source = [jnp.int32(-1)] * 8
    up_row = [jnp.int32(0), jnp.int32(0)]
    down_row = [jnp.int32(0), jnp.int32(0)]
    up_low, up_high = jnp.int32(99), jnp.int32(-1)
    down_low, down_high = jnp.int32(99), jnp.int32(-1)
    for r in range(ROWS):
        bx = pos[0, r]
        layer = bx - 2 * s
        bz = pos[2, r] - 4 * core
        spot = jnp.where((layer >= 0) & (layer < 2) & (bx >= 0), layer * 4 + bz, -1)
        source = [jnp.where(spot == j, r, source[j]) for j in range(8)]
        rises = layer >= 2
        sinks = (layer < 0) & (bx >= 0)
        less, more = rises & (bz < up_low), rises & (bz > up_high)
        up_row = [jnp.where(less, r, up_row[0]), jnp.where(more, r, up_row[1])]
        up_low, up_high = jnp.where(less, bz, up_low), jnp.where(more, bz, up_high)
        less, more = sinks & (bz < down_low), sinks & (bz > down_high)
        down_row = [jnp.where(less, r, down_row[0]), jnp.where(more, r, down_row[1])]
        down_low, down_high = jnp.where(less, bz, down_low), jnp.where(more, bz, down_high)
    order = []
    for layer in range(2):
        missing = jnp.int32(0)
        for z in range(4):
            order.append(jnp.minimum(missing, 1))
            missing = missing + jnp.where(source[layer * 4 + z] < 0, 1, 0)
    here = [jnp.full((8, 128), source[j], jnp.int32) >= 0 for j in range(8)]
    here4 = [jnp.full((4, 128), source[j], jnp.int32) >= 0 for j in range(8)]
    later = [jnp.full((8, 128), order[j], jnp.int32) > 0 for j in range(8)]
    second = [jnp.full((4, 128), order[j], jnp.int32) > 0 for j in range(8)]
    source = [jnp.maximum(source[j], 0) for j in range(8)]

    for load in loads[1:]:
        load.wait()
    for r in range(ROWS):
        held_marks[r] = marks_in[r:r + 1, :].astype(F32)

    def plane_of(pair, side):
        return pair + side * (15 - 2 * pair)

    def cells(k):
        return pl.ds(pl.multiple_of(k * 128, 128), 128)

    def tail(row, k):
        return jnp.concatenate([held[row, 16:19, cells(k)], held_marks[row, :, cells(k)]], axis=0)

    def move(d, c):
        return pltpu.make_async_remote_copy(
            src_ref=send.at[d, c], dst_ref=recv.at[d, c],
            send_sem=move_send.at[d, c], recv_sem=move_recv.at[d, c],
            device_id=partners[d], device_id_type=MESH,
        )

    def pack(c):
        @pl.loop(0, TILES)
        def _(kk):
            k = 2 * plane_of(c, kk // 2) + kk % 2
            for d, rows in ((0, up_row), (1, down_row)):
                for q in range(2):
                    send[d, c, kk, 2 * q] = held[rows[q], 0:8, cells(k)]
                    send[d, c, kk, 2 * q + 1] = held[rows[q], 8:16, cells(k)]
                send[d, c, kk, 4] = jnp.concatenate(
                    [tail(rows[0], k), tail(rows[1], k)], axis=0)

    pack(0)
    pl.semaphore_wait(barrier, arrivals)
    for c in range(CHUNKS):
        if c:
            pack(c)
        for d in range(2):
            when(exists[d], lambda d=d, c=c: move(d, c).start())

    lane = lax.broadcasted_iota(jnp.int32, (8, 128), 1)
    low_half = lane < 64
    flat_lane = lane % 64
    z_edge = jnp.where(core == 0, 63, 0)
    sent_z = [jnp.where(core == 0, group[3], group[4]) for group in GROUPS] + [MARK]

    def count(step):
        return 6 if step == 0 else 5

    def late_planes(step):
        first = OUTER - step
        return first, 16 - 2 * first

    def late_rows(step):
        return -(-count(step) * late_planes(step)[1] // 8) * 8

    def message(step, kind, e):
        n = count(step)
        if kind == "x":
            i, src, dst, slot = e, face_x.at[step, e, pl.ds(0, n)], got_x.at[step, e, pl.ds(0, n)], e
        elif kind == "xy":
            i, src, dst, slot = 5 + e, edge_xy.at[step, e], got_xy.at[step, e], 2 + e
        elif kind == "xz":
            i, src, dst, slot = 11 + e, edge_xz.at[step, e], got_xz.at[step, e], 6 + e
        elif kind == "y0":
            i, src, dst = 2 + e, face_y.at[step, e, pl.ds(0, n)], got_y.at[step, e, pl.ds(0, n)]
            slot = 8 + e
        elif kind == "y1":
            rows = pl.ds(0, late_rows(step))
            i, src, dst = 2 + e, late_y.at[step, e, rows], got_late_y.at[step, e, rows]
            slot = 13 + e
        else:
            g = int(kind[-1])
            if kind[:-1] == "z":
                i, slot = 4, 10 + 5 * g
                src, dst = face_z.at[step, g, pl.ds(0, n)], got_z.at[step, g, pl.ds(0, n)]
            else:
                i, slot = 9 + e, 11 + 5 * g + e
                src, dst = edge_yz.at[step, g, e], got_yz.at[step, g, e]
        copy = pltpu.make_async_remote_copy(
            src_ref=src, dst_ref=dst, send_sem=halo_send.at[step, slot],
            recv_sem=halo_recv.at[step, slot], device_id=partners[i], device_id_type=MESH,
        )
        return copy, exists[i], exists[REVERSE[i]]

    def of_kind(step, *kinds):
        sizes = {"x": 2, "xy": 4, "xz": 2, "y0": 2, "y1": 2, "z0": 1, "z1": 1, "yz0": 2, "yz1": 2}
        return [message(step, kind, e) for kind in kinds for e in range(sizes[kind])]

    def start(step, *kinds):
        for copy, there, _ in of_kind(step, *kinds):
            when(there, copy.start)

    def arrive(step, *kinds):
        for copy, _, there in of_kind(step, *kinds):
            when(there, copy.wait_recv)

    def send_x(ext, step):
        n = count(step)
        for d, pops in ((0, UP_X), (1, DOWN_X)):
            plane = 16 if d == 0 else 1
            for j, p in enumerate((pops + (MARK,))[:n]):
                for h in range(2):
                    face_x[step, d, j, 8 * h:8 * h + 8, :] = roll(
                        ext[p, plane, 8 + 8 * h:16 + 8 * h, :], 64)
        for e, (d, j, row) in enumerate(((0, 1, 15), (1, 1, 0), (0, 2, 0), (1, 2, 15))):
            edge_xy[step, e, 0:1, :] = face_x[step, d, j, row:row + 1, :]
            if step == 0:
                edge_xy[step, e, 1:2, :] = face_x[step, d, 5, row:row + 1, :]
        for e, (j, plane) in enumerate(((1, 16), (2, 1))):
            shift = (64 - z_edge) if e == 0 else (128 + 81 - z_edge) % 128
            for h in range(2):
                rows = slice(8 + 8 * h, 16 + 8 * h)
                value = roll(ext[sent_z[j], plane, rows, :], shift)
                if step == 0:
                    marks = roll(roll(ext[MARK, plane, rows, :], shift), 1)
                    value = jnp.where(lane == (0 if e == 0 else 81), value, marks)
                edge_xz[step, e, 8 * h:8 * h + 8, :] = value
        start(step, "x", "xy", "xz")

    def send_yz(ext, step, late):
        n = count(step)
        flat = ext.reshape(20, 18 * 32, 128)
        first, planes = late_planes(step)
        for d, pops in ((0, UP_Y), (1, DOWN_Y)):
            row = 23 if d == 0 else 8
            for j, p in enumerate((pops + (MARK,))[:n]):
                if late:
                    late_y[step, d, j * planes:(j + 1) * planes, :] = flat[
                        p, pl.ds(32 * (1 + first) + row, planes, stride=32), :]
                else:
                    for h in range(2):
                        face_y[step, d, j, 8 * h:8 * h + 8, :] = flat[
                            p, pl.ds(32 * (1 + 8 * h) + row, 8, stride=32), :]
        start(step, "y1" if late else "y0")

        def gather(i, totals):
            a = first + i if late else i + (i // first) * planes
            shift = lax.rem(a + 1 - z_edge + 128, 128)
            keep = flat_lane == a + 1
            return tuple(
                jnp.where(keep, roll(ext[sent_z[j], a + 1, 8 + 8 * h:16 + 8 * h, :], shift),
                          totals[2 * j + h])
                for j in range(n) for h in range(2)
            )

        zero = jnp.zeros((8, 128), F32)
        totals = lax.fori_loop(0, planes if late else 2 * first, gather, (zero,) * (2 * n))
        for j in range(n):
            for h in range(2):
                face_z[step, late, j, 8 * h:8 * h + 8, :] = totals[2 * j + h]
        for e, (j, row) in enumerate(((3, 15), (4, 0))):
            edge_yz[step, late, e, 0:1, :] = face_z[step, late, j, row:row + 1, :]
            if step == 0:
                edge_yz[step, late, e, 1:2, :] = face_z[step, late, 5, row:row + 1, :]
        start(step, "yz1" if late else "yz0", "z1" if late else "z0")

    def outside_or(condition, value):
        return jnp.where(condition, jnp.full_like(value, 2.0), value)

    def take_yz(ext, step, late):
        n = count(step)
        flat = ext.reshape(20, 18 * 32, 128)
        first, planes = late_planes(step)
        if late:
            arrive(step, "z1", "y1", "yz1")
        else:
            arrive(step, "z0", "y0", "yz0")
        for d, pops, row in ((0, UP_Y, 7), (1, DOWN_Y, 24)):
            outside = (cy == 0) if d == 0 else (cy == n_y - 1)
            for j, p in enumerate((pops + (MARK,))[:n]):
                if late:
                    value = got_late_y[step, d, j * planes:(j + 1) * planes, :]
                    if p == MARK:
                        value = outside_or(outside, value)
                    flat[p, pl.ds(32 * (1 + first) + row, planes, stride=32), :] = value
                else:
                    for h in range(2):
                        value = got_y[step, d, j, 8 * h:8 * h + 8, :]
                        if p == MARK:
                            value = outside_or(outside, value)
                        flat[p, pl.ds(32 * (1 + 8 * h) + row, 8, stride=32), :] = value
        fresh = (flat_lane > first) & (flat_lane <= first + planes)

        def merge(j, rows, value):
            if late:
                value = jnp.where(fresh[0:value.shape[0]], value, zext[step, j, rows, :])
            zext[step, j, rows, :] = value

        for j in range(n):
            for h in range(2):
                value = got_z[step, late, j, 8 * h:8 * h + 8, :]
                if not late:
                    fixed = value
                    if j in (1, 5):
                        fixed = jnp.where(lane == 64, roll(value, 48), fixed)
                    if j in (2, 5):
                        fixed = jnp.where(lane == 17, roll(value, 80), fixed)
                    value = fixed
                merge(j, slice(8 + 8 * h, 16 + 8 * h), value)
        merge(3, slice(7, 8), got_yz[step, late, 0, 0:1, :])
        merge(4, slice(24, 25), got_yz[step, late, 1, 0:1, :])
        if step == 0:
            for e, row in ((0, 7), (1, 24)):
                outside = (cy == 0) if e == 0 else (cy == n_y - 1)
                merge(5, slice(row, row + 1), outside_or(outside, got_yz[step, late, e, 1:2, :]))

    def take_x(ext, step):
        n = count(step)
        arrive(step, "x", "xy", "xz")
        for d, pops in ((0, UP_X), (1, DOWN_X)):
            plane = 0 if d == 0 else 17
            beyond = low_half if d == 0 else jnp.logical_not(low_half)
            outside = (s == 0) if d == 0 else (s == n_s - 1)
            for j, p in enumerate((pops + (MARK,))[:n]):
                for h in range(2):
                    value = got_x[step, d, j, 8 * h:8 * h + 8, :]
                    if p == MARK:
                        value = outside_or(outside, value)
                    ext[p, plane, 8 + 8 * h:16 + 8 * h, :] = jnp.where(
                        beyond, value, face_x[step, d, j, 8 * h:8 * h + 8, :])
        for e, (d, p, row) in enumerate(((0, 7, 7), (1, 8, 24), (0, 9, 24), (1, 10, 7))):
            plane, behind = (0, 16) if d == 0 else (17, 1)
            beyond = (low_half if d == 0 else jnp.logical_not(low_half))[0:1]
            own = roll(ext[p, behind, row:row + 1, :], 64)
            ext[p, plane, row:row + 1, :] = jnp.where(beyond, got_xy[step, e, 0:1, :], own)
            if step == 0:
                out_x = (s == 0) if d == 0 else (s == n_s - 1)
                out_y = (cy == 0) if row == 7 else (cy == n_y - 1)
                value = outside_or(out_x | out_y, got_xy[step, e, 1:2, :])
                own = roll(ext[MARK, behind, row:row + 1, :], 64)
                ext[MARK, plane, row:row + 1, :] = jnp.where(beyond, value, own)
        for e, (j, at) in enumerate(((1, 0), (2, 81))):
            outside = (s == 0) if e == 0 else (s == n_s - 1)
            for h in range(2):
                rows = slice(8 + 8 * h, 16 + 8 * h)
                value = got_xz[step, e, 8 * h:8 * h + 8, :]
                zext[step, j, rows, :] = jnp.where(lane == at, value, zext[step, j, rows, :])
                if step == 0:
                    marks = outside_or(outside, roll(value, -1))
                    zext[step, 5, rows, :] = jnp.where(lane == at, marks, zext[step, 5, rows, :])

    def settle(c, carry):
        for d in range(2):
            when(exists[1 - d], lambda d=d: move(d, c).wait_recv())

        @pl.loop(0, 2)
        def _(side):
            a = plane_of(c, side)
            for h in range(2):
                kk = side * 2 + h
                k = 2 * a + h
                for t in range(3):
                    tiles = []
                    for j in range(8):
                        d = j // 4
                        if t < 2:
                            mine = held[source[j], 8 * t:8 * t + 8, cells(k)]
                            theirs = jnp.where(later[j], recv[d, c, kk, 2 + t], recv[d, c, kk, t])
                            tiles.append(jnp.where(here[j], mine, theirs))
                        else:
                            theirs = recv[d, c, kk, 4]
                            theirs = jnp.where(second[j], theirs[4:8], theirs[0:4])
                            tiles.append(jnp.where(here4[j], tail(source[j], k), theirs))
                    height = tiles[0].shape[0]
                    for g, value in enumerate(group_swap(tiles)):
                        stage[t, 8 * g:8 * g + height, :] = value
                f = [stage[p // 8, pl.ds(p % 8, 8, stride=8), :] for p in range(19)]
                marks = stage[2, pl.ds(3, 8, stride=8), :]
                post, density = collide(f, marks > 0.5)
                for p in range(19):
                    ext1[p, a + 1, 8 + 8 * h:16 + 8 * h, :] = post[p]
                ext1[MARK, a + 1, 8 + 8 * h:16 + 8 * h, :] = marks
                rho[a, 8 * h:8 * h + 8, :] = density

        pl.when(c == 0)(lambda: send_x(ext1, 0))
        pl.when(c == OUTER - 1)(lambda: send_yz(ext1, 0, 0))
        return carry

    lax.fori_loop(0, CHUNKS, settle, 0)
    send_yz(ext1, 0, 1)

    first_z = flat_lane == 0
    last_z = flat_lane == 63
    z_target = jnp.where(core == 1, 0, 63)

    def rows(h, step_y):
        start_row = 8 + 8 * h - step_y
        return slice(start_row, start_row + 8)

    def z_halo(step, j, a, h, step_x, step_y):
        shift = lax.rem(z_target - a + (127 + step_x), 128)
        return roll(zext[step, j, rows(h, step_y), :], shift)

    def make_bits(a, h):
        wall = jnp.zeros((8, 128), jnp.int32)
        rotor = jnp.zeros((8, 128), jnp.int32)

        def add(bit, value):
            nonlocal wall, rotor
            wall = wall + jnp.where(value > 0.5, 1 << bit, 0)
            if bit > 2:
                rotor = rotor + jnp.where(value == 1.0, 1 << bit, 0)

        for step_x, step_y, p_flat, p_up, p_down in GROUPS:
            value = ext1[MARK, a + 1 - step_x, rows(h, step_y), :]
            add(p_flat, value)
            halo = z_halo(0, 5, a, h, step_x, step_y)
            add(p_up, jnp.where(first_z, outside_or(core == 0, halo), roll(value, 1)))
            add(p_down, jnp.where(last_z, outside_or(core == 1, halo), roll(value, -1)))
        for step_x, step_y, p in DIAGONALS:
            add(p, ext1[MARK, a + 1 - step_x, rows(h, step_y), :])
        walls[a, 8 * h:8 * h + 8, :] = wall
        rotors[a, 8 * h:8 * h + 8, :] = rotor
        return wall, rotor

    along_z = (core * 64 + flat_lane).astype(F32) - 63.5
    drift_a = (-OMEGA / 6.0) * along_z
    sub = lax.broadcasted_iota(jnp.int32, (8, 128), 0)

    def pull(ext, step, a, h, wall, rotor):
        here_rows = slice(8 + 8 * h, 16 + 8 * h)
        centre = [ext[p, a + 1, here_rows, :] for p in range(19)]
        density = rho[a, 8 * h:8 * h + 8, :]
        along_y = (cy * 16 + 8 * h + sub).astype(F32) - 31.5
        push_a = density * drift_a
        push_b = density * ((OMEGA / 6.0) * along_y)
        both, apart = push_a + push_b, push_a - push_b
        push = {
            3: 2.0 * push_a, 4: -2.0 * push_a, 5: 2.0 * push_b, 6: -2.0 * push_b,
            7: push_a, 8: -push_a, 9: -push_a, 10: push_a,
            11: push_b, 12: -push_b, 13: -push_b, 14: push_b,
            15: both, 16: -both, 17: apart, 18: -apart,
        }
        solid = (wall & 1) != 0
        new = [None] * 19
        new[0] = centre[0]

        def settle_one(p, pulled):
            bounced = centre[OPPOSITE[p]]
            if p > 2:
                bounced = bounced + jnp.where((rotor & (1 << p)) != 0, push[p], 0.0)
            value = jnp.where((wall & (1 << p)) != 0, bounced, pulled)
            new[p] = jnp.where(solid, centre[p], value)

        for j, (step_x, step_y, p_flat, p_up, p_down) in enumerate(GROUPS):
            if p_flat:
                settle_one(p_flat, ext[p_flat, a + 1 - step_x, rows(h, step_y), :])
            halo = z_halo(step, j, a, h, step_x, step_y)
            value = ext[p_up, a + 1 - step_x, rows(h, step_y), :]
            settle_one(p_up, jnp.where(first_z, halo, roll(value, 1)))
            value = ext[p_down, a + 1 - step_x, rows(h, step_y), :]
            settle_one(p_down, jnp.where(last_z, halo, roll(value, -1)))
        for step_x, step_y, p in DIAGONALS:
            settle_one(p, ext[p, a + 1 - step_x, rows(h, step_y), :])
        return new, solid

    take_yz(ext1, 0, 0)
    take_x(ext1, 0)

    def middle(i, carry):
        @pl.when(i == 2)
        def _():
            send_x(ext2, 1)

        @pl.when(i == 2 * (OUTER - 1))
        def _():
            send_yz(ext2, 1, 0)
            take_yz(ext1, 0, 1)

        a = plane_of(i // 2, i % 2)
        for h in range(2):
            wall, rotor = make_bits(a, h)
            new, solid = pull(ext1, 0, a, h, wall, rotor)
            post, density = collide(new, solid)
            for p in range(19):
                ext2[p, a + 1, 8 + 8 * h:16 + 8 * h, :] = post[p]
            rho[a, 8 * h:8 * h + 8, :] = density
        return carry

    lax.fori_loop(0, EDGE, middle, 0)
    send_yz(ext2, 1, 1)
    take_yz(ext2, 1, 0)

    def last(i, carry):
        @pl.when(i == 2 * (OUTER - 3))
        def _():
            take_yz(ext2, 1, 1)

        @pl.when(i == 14)
        def _():
            take_x(ext2, 1)

        a = plane_of((i // 2 + 1) % 8, i % 2)
        for h in range(2):
            wall = walls[a, 8 * h:8 * h + 8, :]
            rotor = rotors[a, 8 * h:8 * h + 8, :]
            new, _ = pull(ext2, 1, a, h, wall, rotor)
            for p in range(19):
                out[p, a, 8 * h:8 * h + 8, :] = new[p][:, 0:64]
                out[p, EDGE + a, 8 * h:8 * h + 8, :] = roll(new[p], 64)[:, 0:64]
        return carry

    lax.fori_loop(0, EDGE, last, 0)
    for c in range(CHUNKS):
        for d in range(2):
            when(exists[d], lambda d=d, c=c: move(d, c).wait_send())
    for step in range(2):
        for copy, there, _ in of_kind(step, "x", "xy", "xz", "y0", "y1", "z0", "z1", "yz0", "yz1"):
            when(there, copy.wait_send)


def step_all(populations, solid_cells, block_pos):
    scratch = [
        pltpu.VMEM((ROWS, 19, 4096), F32),
        pltpu.VMEM((ROWS, 4096), jnp.int32),
        pltpu.VMEM((ROWS, 1, 4096), F32),
        pltpu.SMEM((3, ROWS), jnp.int32),
        pltpu.VMEM((2, CHUNKS, TILES, 5, 8, 128), F32),
        pltpu.VMEM((2, CHUNKS, TILES, 5, 8, 128), F32),
        pltpu.VMEM((3, 64, 128), F32),
        pltpu.VMEM((20, 18, 32, 128), F32),
        pltpu.VMEM((20, 18, 32, 128), F32),
        pltpu.VMEM((EDGE, 16, 128), F32),
        pltpu.VMEM((EDGE, 16, 128), jnp.int32),
        pltpu.VMEM((EDGE, 16, 128), jnp.int32),
    ]
    for _ in range(2):
        scratch += [
            pltpu.VMEM((2, 2, 6, 16, 128), F32),
            pltpu.VMEM((2, 2, 6, 16, 128), F32),
            pltpu.VMEM((2, 2, 48, 128), F32),
            pltpu.VMEM((2, 2, 6, 16, 128), F32),
            pltpu.VMEM((2, 4, 8, 128), F32),
            pltpu.VMEM((2, 2, 2, 8, 128), F32),
            pltpu.VMEM((2, 2, 16, 128), F32),
        ]
    scratch += [
        pltpu.VMEM((2, 6, 32, 128), F32),
        pltpu.SemaphoreType.DMA((6,)),
        pltpu.SemaphoreType.DMA((2, CHUNKS)),
        pltpu.SemaphoreType.DMA((2, CHUNKS)),
        pltpu.SemaphoreType.DMA((2, 18)),
        pltpu.SemaphoreType.DMA((2, 18)),
    ]
    return pl.pallas_call(
        kernel,
        out_shape=jax.ShapeDtypeStruct((19, 32, 16, 64), F32),
        in_specs=[pl.BlockSpec(memory_space=pltpu.HBM)] * 3,
        out_specs=pl.BlockSpec(memory_space=pltpu.VMEM),
        scratch_shapes=scratch,
        compiler_params=pltpu.CompilerParams(
            collective_id=0, has_side_effects=True, vmem_limit_bytes=40 * 1024 * 1024
        ),
    )(*(pltpu.with_memory_space_constraint(value, pltpu.HBM)
        for value in (block_pos.T, populations, solid_cells)))


def solution(mesh):
    in_specs = (
        P(("stream", "cy", "cz"), None, None),
        P(("stream", "cy", "cz"), None),
        P(("stream", "cy", "cz"), None),
    )
    out_specs = P(None, "stream", "cy", "cz")
    return jax.shard_map(step_all, mesh=mesh, in_specs=in_specs, out_specs=out_specs, check_vma=False)
```

```python
import jax
import jax.numpy as jnp
from jax import lax
from jax.experimental import pallas as pl
from jax.experimental.pallas import tpu as pltpu
from jax.sharding import PartitionSpec as P

MESH = pl.DeviceIdType.MESH
F32 = jnp.float32

GROUPS = (
    (0, 0, 0, 5, 6),
    (1, 0, 1, 11, 13),
    (-1, 0, 2, 14, 12),
    (0, 1, 3, 15, 17),
    (0, -1, 4, 18, 16),
)
DIAGONALS = ((1, 1, 7), (-1, -1, 8), (1, -1, 9), (-1, 1, 10))
PAIRS = ((1, 2), (3, 4), (5, 6), (7, 8), (9, 10), (11, 12), (13, 14), (15, 16), (17, 18))
OPPOSITE = (0, 2, 1, 4, 3, 6, 5, 8, 7, 10, 9, 12, 11, 14, 13, 16, 15, 18, 17)
UP_X = (1, 7, 9, 11, 13)
DOWN_X = (2, 8, 10, 12, 14)
UP_Y = (3, 7, 10, 15, 17)
DOWN_Y = (4, 8, 9, 16, 18)
MARK = 19

EDGE = 16
CHUNKS = 8
TILES = 4
ROWS = 12
OMEGA = 0.2 / 192.0
REVERSE = (1, 0, 3, 2, 4, 6, 5, 8, 7, 10, 9, 12, 11)


def roll(value, shift, axis=1):
    return pltpu.roll(value, shift % value.shape[axis] if isinstance(shift, int) else shift, axis)


def collide(f, mark):
    plus = [f[i] + f[o] for i, o in PAIRS]
    minus = [f[i] - f[o] for i, o in PAIRS]
    density = f[0] + ((plus[0] + plus[1]) + (plus[2] + plus[3])) + (
        (plus[4] + plus[5]) + (plus[6] + plus[7]) + plus[8]
    )
    mx = (minus[0] + minus[3]) + (minus[4] + minus[5]) + minus[6]
    my = (minus[1] + minus[3]) - (minus[4] - minus[7]) + minus[8]
    mz = (minus[2] + minus[5]) - (minus[6] - minus[7]) - minus[8]
    inverse = 1.0 / density
    base = density - 1.5 * (mx * mx + my * my + mz * mz) * inverse
    squared = 4.5 * inverse
    along = (mx, my, mz, mx + my, mx - my, mx + mz, mx - mz, my + mz, my - mz)
    post = [None] * 19
    post[0] = f[0] - 1.25 * (f[0] - (1.0 / 3.0) * base)
    for k, (i, o) in enumerate(PAIRS):
        weight = 1.0 / 18.0 if k < 3 else 1.0 / 36.0
        m = along[k]
        even = 0.625 * plus[k] - (1.25 * weight) * (base + squared * (m * m))
        odd = (4.0 / 9.0) * minus[k] - (8.0 / 3.0 * weight) * m
        post[i] = f[i] - even - odd
        post[o] = f[o] - even + odd
    return [jnp.where(mark, f[i], post[i]) for i in range(19)], density


def group_swap(values):
    lane = lax.broadcasted_iota(jnp.int32, values[0].shape, 1)
    for bit in range(3):
        step = 1 << bit
        high = (lane // (16 * step)) % 2 == 1
        out = list(values)
        for i in range(8):
            if i & step:
                continue
            low_one, high_one = values[i], values[i + step]
            out[i] = jnp.where(high, roll(high_one, 16 * step), low_one)
            out[i + step] = jnp.where(high, high_one, roll(low_one, -16 * step))
        values = out
    return values


def kernel(pos_in, pop_in, mark_in, out, held, marks_in, held_marks, pos, send, recv, stage, ext1, ext2,
           rho, walls, rotors, face_x, face_y, face_z, edge_xy, edge_yz, edge_xz,
           got_x, got_y, got_z, got_xy, got_yz, got_xz, zext,
           in_sem, move_send, move_recv, x_send, x_recv, pair_send, pair_recv):
    s = lax.axis_index("stream")
    cy = lax.axis_index("cy")
    core = lax.axis_index("cz")
    n_s = lax.axis_size("stream")
    n_y = lax.axis_size("cy")
    up_s, down_s = lax.rem(s + 1, n_s), lax.rem(s + n_s - 1, n_s)
    up_y, down_y = lax.rem(cy + 1, n_y), lax.rem(cy + n_y - 1, n_y)
    other = 1 - core
    partners = (
        (up_s, cy, core), (down_s, cy, core), (s, up_y, core), (s, down_y, core), (s, cy, other),
        (up_s, up_y, core), (down_s, down_y, core), (up_s, down_y, core), (down_s, up_y, core),
        (s, up_y, other), (s, down_y, other), (up_s, cy, other), (down_s, cy, other),
    )
    above_s, below_s = s < n_s - 1, s > 0
    above_y, below_y = cy < n_y - 1, cy > 0
    exists = (
        above_s, below_s, above_y, below_y, None,
        above_s & above_y, below_s & below_y, above_s & below_y, below_s & above_y,
        above_y, below_y, above_s, below_s,
    )

    def when(condition, act):
        if condition is None:
            act()
        else:
            pl.when(condition)(act)

    loads = [pltpu.make_async_copy(pos_in, pos, in_sem.at[0]),
             pltpu.make_async_copy(mark_in, marks_in, in_sem.at[1])]
    loads += [
        pltpu.make_async_copy(pop_in.at[pl.ds(3 * i, 3)], held.at[pl.ds(3 * i, 3)], in_sem.at[2 + i])
        for i in range(4)
    ]
    for load in loads:
        load.start()
    barrier = pltpu.get_barrier_semaphore()
    arrivals = jnp.int32(0)
    for i, partner in enumerate(partners):
        when(exists[i], lambda partner=partner: pl.semaphore_signal(
            barrier, inc=1, device_id=partner, device_id_type=MESH))
        arrivals = arrivals + (1 if exists[i] is None else jnp.where(exists[i], 1, 0))

    loads[0].wait()
    source = [jnp.int32(-1)] * 8
    up_row = [jnp.int32(0), jnp.int32(0)]
    down_row = [jnp.int32(0), jnp.int32(0)]
    up_low, up_high = jnp.int32(99), jnp.int32(-1)
    down_low, down_high = jnp.int32(99), jnp.int32(-1)
    for r in range(ROWS):
        bx = pos[0, r]
        layer = bx - 2 * s
        bz = pos[2, r] - 4 * core
        spot = jnp.where((layer >= 0) & (layer < 2) & (bx >= 0), layer * 4 + bz, -1)
        source = [jnp.where(spot == j, r, source[j]) for j in range(8)]
        rises = layer >= 2
        sinks = (layer < 0) & (bx >= 0)
        less, more = rises & (bz < up_low), rises & (bz > up_high)
        up_row = [jnp.where(less, r, up_row[0]), jnp.where(more, r, up_row[1])]
        up_low, up_high = jnp.where(less, bz, up_low), jnp.where(more, bz, up_high)
        less, more = sinks & (bz < down_low), sinks & (bz > down_high)
        down_row = [jnp.where(less, r, down_row[0]), jnp.where(more, r, down_row[1])]
        down_low, down_high = jnp.where(less, bz, down_low), jnp.where(more, bz, down_high)
    order = []
    for layer in range(2):
        missing = jnp.int32(0)
        for z in range(4):
            order.append(jnp.minimum(missing, 1))
            missing = missing + jnp.where(source[layer * 4 + z] < 0, 1, 0)
    here = [jnp.full((8, 128), source[j], jnp.int32) >= 0 for j in range(8)]
    here4 = [jnp.full((4, 128), source[j], jnp.int32) >= 0 for j in range(8)]
    later = [jnp.full((8, 128), order[j], jnp.int32) > 0 for j in range(8)]
    second = [jnp.full((4, 128), order[j], jnp.int32) > 0 for j in range(8)]
    source = [jnp.maximum(source[j], 0) for j in range(8)]

    for load in loads[1:]:
        load.wait()
    for r in range(ROWS):
        held_marks[r] = marks_in[r:r + 1, :].astype(F32)

    def plane_of(pair, side):
        return pair + side * (15 - 2 * pair)

    def cells(k):
        return pl.ds(pl.multiple_of(k * 128, 128), 128)

    def tail(row, k):
        return jnp.concatenate([held[row, 16:19, cells(k)], held_marks[row, :, cells(k)]], axis=0)

    def move(d, c):
        return pltpu.make_async_remote_copy(
            src_ref=send.at[d, c], dst_ref=recv.at[d, c],
            send_sem=move_send.at[d, c], recv_sem=move_recv.at[d, c],
            device_id=partners[d], device_id_type=MESH,
        )

    def pack(c):
        @pl.loop(0, TILES)
        def _(kk):
            k = 2 * plane_of(c, kk // 2) + kk % 2
            for d, rows in ((0, up_row), (1, down_row)):
                for q in range(2):
                    send[d, c, kk, 2 * q] = held[rows[q], 0:8, cells(k)]
                    send[d, c, kk, 2 * q + 1] = held[rows[q], 8:16, cells(k)]
                send[d, c, kk, 4] = jnp.concatenate(
                    [tail(rows[0], k), tail(rows[1], k)], axis=0)

    pack(0)
    pl.semaphore_wait(barrier, arrivals)
    for c in range(CHUNKS):
        if c:
            pack(c)
        for d in range(2):
            when(exists[d], lambda d=d, c=c: move(d, c).start())

    lane = lax.broadcasted_iota(jnp.int32, (8, 128), 1)
    low_half = lane < 64
    flat_lane = lane % 64
    z_edge = jnp.where(core == 0, 63, 0)
    sent_z = [jnp.where(core == 0, group[3], group[4]) for group in GROUPS] + [MARK]
    edge_shift = [lax.rem(128 + j - z_edge, 128) for j in range(6)]

    def count(step):
        return 6 if step == 0 else 5

    def remote(src, dst, sems, i):
        copy = pltpu.make_async_remote_copy(
            src_ref=src, dst_ref=dst, send_sem=sems[0], recv_sem=sems[1],
            device_id=partners[i], device_id_type=MESH,
        )
        return copy, exists[i], exists[REVERSE[i]]

    def x_messages(step):
        n = count(step)
        refs = [(face_x.at[step, d, pl.ds(0, n)], got_x.at[step, d, pl.ds(0, n)], d) for d in range(2)]
        refs += [(edge_xy.at[step, e], got_xy.at[step, e], 5 + e) for e in range(4)]
        refs += [(edge_xz.at[step, e], got_xz.at[step, e], 11 + e) for e in range(2)]
        return [
            remote(src, dst, (x_send.at[step, k], x_recv.at[step, k]), i)
            for k, (src, dst, i) in enumerate(refs)
        ]

    def pair_messages(step, c):
        refs = [(face_y.at[step, c, d], got_y.at[step, c, d], 2 + d) for d in range(2)]
        refs += [(edge_yz.at[step, c, d], got_yz.at[step, c, d], 9 + d) for d in range(2)]
        refs += [(face_z.at[step, c], got_z.at[step, c], 4)]
        return [
            remote(src, dst, (pair_send.at[step, c, k], pair_recv.at[step, c, k]), i)
            for k, (src, dst, i) in enumerate(refs)
        ]

    def start(copies):
        for copy, there, _ in copies:
            when(there, copy.start)

    def arrive(copies):
        for copy, _, there in copies:
            when(there, copy.wait_recv)

    def outside_or(condition, value):
        return jnp.where(condition, jnp.full_like(value, 2.0), value)

    def pack_plane(ext, step, c, side, a):
        n = count(step)
        for d, pops in ((0, UP_Y), (1, DOWN_Y)):
            row = 23 if d == 0 else 8
            for j, p in enumerate((pops + (MARK,))[:n]):
                face_y[step, c, d, side, j:j + 1, :] = ext[p, a + 1, row:row + 1, :]
        for h in range(2):
            column = jnp.zeros((8, 128), F32)
            for j in range(n):
                value = ext[sent_z[j], a + 1, 8 + 8 * h:16 + 8 * h, :]
                column = jnp.where(flat_lane == j, roll(value, edge_shift[j]), column)
            face_z[step, c, side, 8 * h:8 * h + 8, :] = column
            if h == 0:
                edge_yz[step, c, 1, side, 0:1, :] = column[0:1]
            else:
                edge_yz[step, c, 0, side, 0:1, :] = column[7:8]

    def take_pair(ext, step, c):
        n = count(step)
        arrive(pair_messages(step, c))
        for side in range(2):
            a = plane_of(c, side)
            for d, pops, row in ((0, UP_Y, 7), (1, DOWN_Y, 24)):
                outside = (cy == 0) if d == 0 else (cy == n_y - 1)
                for j, p in enumerate((pops + (MARK,))[:n]):
                    value = got_y[step, c, d, side, j:j + 1, :]
                    if p == MARK:
                        value = outside_or(outside, value)
                    ext[p, a + 1, row:row + 1, :] = value
                value = got_yz[step, c, d, side, 0:1, :]
                if step == 0:
                    value = jnp.where(flat_lane[0:1] == 5, outside_or(outside, value), value)
                zext[step, a + 1, row:row + 1, :] = value
            for h in range(2):
                zext[step, a + 1, 8 + 8 * h:16 + 8 * h, :] = got_z[
                    step, c, side, 8 * h:8 * h + 8, :]

    def send_x(ext, step):
        n = count(step)
        for d, pops in ((0, UP_X), (1, DOWN_X)):
            plane = 16 if d == 0 else 1
            for j, p in enumerate((pops + (MARK,))[:n]):
                for h in range(2):
                    face_x[step, d, j, 8 * h:8 * h + 8, :] = roll(
                        ext[p, plane, 8 + 8 * h:16 + 8 * h, :], 64)
            for h in range(2):
                edge_xz[step, d, 8 * h:8 * h + 8, :] = roll(
                    face_z[step, 0, 1 - d, 8 * h:8 * h + 8, :], 64)
        for e, (d, j, row) in enumerate(((0, 1, 15), (1, 1, 0), (0, 2, 0), (1, 2, 15))):
            edge_xy[step, e, 0:1, :] = face_x[step, d, j, row:row + 1, :]
            if step == 0:
                edge_xy[step, e, 1:2, :] = face_x[step, d, 5, row:row + 1, :]
        start(x_messages(step))

    def take_x(ext, step):
        n = count(step)
        arrive(x_messages(step))
        for d, pops in ((0, UP_X), (1, DOWN_X)):
            plane, behind = (0, 16) if d == 0 else (17, 1)
            beyond = low_half if d == 0 else jnp.logical_not(low_half)
            outside = (s == 0) if d == 0 else (s == n_s - 1)
            for h in range(2):
                rows = slice(8 + 8 * h, 16 + 8 * h)
                for j, p in enumerate((pops + (MARK,))[:n]):
                    value = got_x[step, d, j, 8 * h:8 * h + 8, :]
                    if p == MARK:
                        value = outside_or(outside, value)
                    ext[p, plane, rows, :] = jnp.where(
                        beyond, value, face_x[step, d, j, 8 * h:8 * h + 8, :])
                value = got_xz[step, d, 8 * h:8 * h + 8, :]
                if step == 0:
                    value = jnp.where(flat_lane == 5, outside_or(outside, value), value)
                zext[step, plane, rows, :] = jnp.where(
                    beyond, value, roll(zext[step, behind, rows, :], 64))
        for e, (d, p, row) in enumerate(((0, 7, 7), (1, 8, 24), (0, 9, 24), (1, 10, 7))):
            plane, behind = (0, 16) if d == 0 else (17, 1)
            beyond = (low_half if d == 0 else jnp.logical_not(low_half))[0:1]
            own = roll(ext[p, behind, row:row + 1, :], 64)
            ext[p, plane, row:row + 1, :] = jnp.where(beyond, got_xy[step, e, 0:1, :], own)
            if step == 0:
                out_x = (s == 0) if d == 0 else (s == n_s - 1)
                out_y = (cy == 0) if row == 7 else (cy == n_y - 1)
                value = outside_or(out_x | out_y, got_xy[step, e, 1:2, :])
                own = roll(ext[MARK, behind, row:row + 1, :], 64)
                ext[MARK, plane, row:row + 1, :] = jnp.where(beyond, value, own)

    def settle(c):
        for d in range(2):
            when(exists[1 - d], lambda d=d: move(d, c).wait_recv())

        @pl.loop(0, 2)
        def _(side):
            a = plane_of(c, side)
            for h in range(2):
                kk = side * 2 + h
                k = 2 * a + h
                for t in range(3):
                    tiles = []
                    for j in range(8):
                        d = j // 4
                        if t < 2:
                            mine = held[source[j], 8 * t:8 * t + 8, cells(k)]
                            theirs = jnp.where(later[j], recv[d, c, kk, 2 + t], recv[d, c, kk, t])
                            tiles.append(jnp.where(here[j], mine, theirs))
                        else:
                            theirs = recv[d, c, kk, 4]
                            theirs = jnp.where(second[j], theirs[4:8], theirs[0:4])
                            tiles.append(jnp.where(here4[j], tail(source[j], k), theirs))
                    height = tiles[0].shape[0]
                    for g, value in enumerate(group_swap(tiles)):
                        stage[t, 8 * g:8 * g + height, :] = value
                f = [stage[p // 8, pl.ds(p % 8, 8, stride=8), :] for p in range(19)]
                marks = stage[2, pl.ds(3, 8, stride=8), :]
                post, density = collide(f, marks > 0.5)
                for p in range(19):
                    ext1[p, a + 1, 8 + 8 * h:16 + 8 * h, :] = post[p]
                ext1[MARK, a + 1, 8 + 8 * h:16 + 8 * h, :] = marks
                rho[a, 8 * h:8 * h + 8, :] = density
            pack_plane(ext1, 0, c, side, a)

        start(pair_messages(0, c))
        pl.when(c == 0)(lambda: send_x(ext1, 0))

    first_z = flat_lane == 0
    last_z = flat_lane == 63
    z_target = jnp.where(core == 1, 0, 63)

    def rows(h, step_y):
        start_row = 8 + 8 * h - step_y
        return slice(start_row, start_row + 8)

    halo_shift = [lax.rem(128 + z_target - j, 128) for j in range(6)]

    def z_halo(step, j, a, h, step_x, step_y):
        return roll(zext[step, a + 1 - step_x, rows(h, step_y), :], halo_shift[j])

    def make_bits(a, h):
        wall = jnp.zeros((8, 128), jnp.int32)
        rotor = jnp.zeros((8, 128), jnp.int32)

        def add(bit, value):
            nonlocal wall, rotor
            wall = wall + jnp.where(value > 0.5, 1 << bit, 0)
            if bit > 2:
                rotor = rotor + jnp.where(value == 1.0, 1 << bit, 0)

        for step_x, step_y, p_flat, p_up, p_down in GROUPS:
            value = ext1[MARK, a + 1 - step_x, rows(h, step_y), :]
            add(p_flat, value)
            halo = z_halo(0, 5, a, h, step_x, step_y)
            add(p_up, jnp.where(first_z, outside_or(core == 0, halo), roll(value, 1)))
            add(p_down, jnp.where(last_z, outside_or(core == 1, halo), roll(value, -1)))
        for step_x, step_y, p in DIAGONALS:
            add(p, ext1[MARK, a + 1 - step_x, rows(h, step_y), :])
        walls[a, 8 * h:8 * h + 8, :] = wall
        rotors[a, 8 * h:8 * h + 8, :] = rotor
        return wall, rotor

    along_z = (core * 64 + flat_lane).astype(F32) - 63.5
    drift_a = (-OMEGA / 6.0) * along_z
    sub = lax.broadcasted_iota(jnp.int32, (8, 128), 0)

    def pull(ext, step, a, h, wall, rotor):
        here_rows = slice(8 + 8 * h, 16 + 8 * h)
        centre = [ext[p, a + 1, here_rows, :] for p in range(19)]
        density = rho[a, 8 * h:8 * h + 8, :]
        along_y = (cy * 16 + 8 * h + sub).astype(F32) - 31.5
        push_a = density * drift_a
        push_b = density * ((OMEGA / 6.0) * along_y)
        both, apart = push_a + push_b, push_a - push_b
        push = {
            3: 2.0 * push_a, 4: -2.0 * push_a, 5: 2.0 * push_b, 6: -2.0 * push_b,
            7: push_a, 8: -push_a, 9: -push_a, 10: push_a,
            11: push_b, 12: -push_b, 13: -push_b, 14: push_b,
            15: both, 16: -both, 17: apart, 18: -apart,
        }
        solid = (wall & 1) != 0
        new = [None] * 19
        new[0] = centre[0]

        def settle_one(p, pulled):
            bounced = centre[OPPOSITE[p]]
            if p > 2:
                bounced = bounced + jnp.where((rotor & (1 << p)) != 0, push[p], 0.0)
            value = jnp.where((wall & (1 << p)) != 0, bounced, pulled)
            new[p] = jnp.where(solid, centre[p], value)

        for j, (step_x, step_y, p_flat, p_up, p_down) in enumerate(GROUPS):
            if p_flat:
                settle_one(p_flat, ext[p_flat, a + 1 - step_x, rows(h, step_y), :])
            halo = z_halo(step, j, a, h, step_x, step_y)
            value = ext[p_up, a + 1 - step_x, rows(h, step_y), :]
            settle_one(p_up, jnp.where(first_z, halo, roll(value, 1)))
            value = ext[p_down, a + 1 - step_x, rows(h, step_y), :]
            settle_one(p_down, jnp.where(last_z, halo, roll(value, -1)))
        for step_x, step_y, p in DIAGONALS:
            settle_one(p, ext[p, a + 1 - step_x, rows(h, step_y), :])
        return new, solid

    def middle(c):
        @pl.when(c == 0)
        def _():
            take_pair(ext1, 0, 0)
            take_x(ext1, 0)

        pl.when(c < CHUNKS - 1)(lambda: take_pair(ext1, 0, c + 1))

        @pl.loop(0, 2)
        def _(side):
            a = plane_of(c, side)
            for h in range(2):
                wall, rotor = make_bits(a, h)
                new, solid = pull(ext1, 0, a, h, wall, rotor)
                post, density = collide(new, solid)
                for p in range(19):
                    ext2[p, a + 1, 8 + 8 * h:16 + 8 * h, :] = post[p]
                rho[a, 8 * h:8 * h + 8, :] = density
            pack_plane(ext2, 1, c, side, a)

        start(pair_messages(1, c))
        pl.when(c == 0)(lambda: send_x(ext2, 1))

    def last(c):
        @pl.when(c == 0)
        def _():
            take_pair(ext2, 1, 0)
            take_x(ext2, 1)

        pl.when(c < CHUNKS - 1)(lambda: take_pair(ext2, 1, c + 1))

        @pl.loop(0, 2)
        def _(side):
            a = plane_of(c, side)
            for h in range(2):
                wall = walls[a, 8 * h:8 * h + 8, :]
                rotor = rotors[a, 8 * h:8 * h + 8, :]
                new, _ = pull(ext2, 1, a, h, wall, rotor)
                for p in range(19):
                    out[p, a, 8 * h:8 * h + 8, :] = new[p][:, 0:64]
                    out[p, EDGE + a, 8 * h:8 * h + 8, :] = roll(new[p], 64)[:, 0:64]

    def collided(t):
        return jnp.where(t >= 9, 8, jnp.clip(t - 2, 0, 6))

    def streamed(t):
        return jnp.where(t >= 10, 8, jnp.clip(t - 5, 0, 4))

    def tick(t, carry):
        @pl.loop(streamed(t - 1), streamed(t))
        def _(c):
            last(c)

        pl.when(t < CHUNKS)(lambda: settle(t))

        @pl.loop(collided(t - 1), collided(t))
        def _(c):
            middle(c)

        return carry

    lax.fori_loop(0, 11, tick, 0)
    for c in range(CHUNKS):
        for d in range(2):
            when(exists[d], lambda d=d, c=c: move(d, c).wait_send())
    for step in range(2):
        for copy, there, _ in x_messages(step):
            when(there, copy.wait_send)
        for c in range(CHUNKS):
            for copy, there, _ in pair_messages(step, c):
                when(there, copy.wait_send)


def step_all(populations, solid_cells, block_pos):
    scratch = [
        pltpu.VMEM((ROWS, 19, 4096), F32),
        pltpu.VMEM((ROWS, 4096), jnp.int32),
        pltpu.VMEM((ROWS, 1, 4096), F32),
        pltpu.SMEM((3, ROWS), jnp.int32),
        pltpu.VMEM((2, CHUNKS, TILES, 5, 8, 128), F32),
        pltpu.VMEM((2, CHUNKS, TILES, 5, 8, 128), F32),
        pltpu.VMEM((3, 64, 128), F32),
        pltpu.VMEM((20, 18, 32, 128), F32),
        pltpu.VMEM((20, 18, 32, 128), F32),
        pltpu.VMEM((EDGE, 16, 128), F32),
        pltpu.VMEM((EDGE, 16, 128), jnp.int32),
        pltpu.VMEM((EDGE, 16, 128), jnp.int32),
    ]
    for _ in range(2):
        scratch += [
            pltpu.VMEM((2, 2, 6, 16, 128), F32),
            pltpu.VMEM((2, CHUNKS, 2, 2, 8, 128), F32),
            pltpu.VMEM((2, CHUNKS, 2, 16, 128), F32),
            pltpu.VMEM((2, 4, 8, 128), F32),
            pltpu.VMEM((2, CHUNKS, 2, 2, 8, 128), F32),
            pltpu.VMEM((2, 2, 16, 128), F32),
        ]
    scratch += [
        pltpu.VMEM((2, 18, 32, 128), F32),
        pltpu.SemaphoreType.DMA((6,)),
        pltpu.SemaphoreType.DMA((2, CHUNKS)),
        pltpu.SemaphoreType.DMA((2, CHUNKS)),
        pltpu.SemaphoreType.DMA((2, 8)),
        pltpu.SemaphoreType.DMA((2, 8)),
        pltpu.SemaphoreType.DMA((2, CHUNKS, 5)),
        pltpu.SemaphoreType.DMA((2, CHUNKS, 5)),
    ]
    return pl.pallas_call(
        kernel,
        out_shape=jax.ShapeDtypeStruct((19, 32, 16, 64), F32),
        in_specs=[pl.BlockSpec(memory_space=pltpu.HBM)] * 3,
        out_specs=pl.BlockSpec(memory_space=pltpu.VMEM),
        scratch_shapes=scratch,
        compiler_params=pltpu.CompilerParams(
            collective_id=0, has_side_effects=True, vmem_limit_bytes=40 * 1024 * 1024
        ),
    )(*(pltpu.with_memory_space_constraint(value, pltpu.HBM)
        for value in (block_pos.T, populations, solid_cells)))


def solution(mesh):
    in_specs = (
        P(("stream", "cy", "cz"), None, None),
        P(("stream", "cy", "cz"), None),
        P(("stream", "cy", "cz"), None),
    )
    out_specs = P(None, "stream", "cy", "cz")
    return jax.shard_map(step_all, mesh=mesh, in_specs=in_specs, out_specs=out_specs, check_vma=False)
```

```python
import jax
import jax.numpy as jnp
from jax import lax
from jax.experimental import pallas as pl
from jax.experimental.pallas import tpu as pltpu
from jax.sharding import PartitionSpec as P

MESH = pl.DeviceIdType.MESH
F32 = jnp.float32

GROUPS = (
    (0, 0, 0, 5, 6),
    (1, 0, 1, 11, 13),
    (-1, 0, 2, 14, 12),
    (0, 1, 3, 15, 17),
    (0, -1, 4, 18, 16),
)
DIAGONALS = ((1, 1, 7), (-1, -1, 8), (1, -1, 9), (-1, 1, 10))
PAIRS = ((1, 2), (3, 4), (5, 6), (7, 8), (9, 10), (11, 12), (13, 14), (15, 16), (17, 18))
OPPOSITE = (0, 2, 1, 4, 3, 6, 5, 8, 7, 10, 9, 12, 11, 14, 13, 16, 15, 18, 17)
UP_X = (1, 7, 9, 11, 13)
DOWN_X = (2, 8, 10, 12, 14)
UP_Y = (3, 7, 10, 15, 17)
DOWN_Y = (4, 8, 9, 16, 18)
MARK = 19

EDGE = 16
CHUNKS = 8
TILES = 4
ROWS = 12
OMEGA = 0.2 / 192.0
REVERSE = (1, 0, 3, 2, 4, 6, 5, 8, 7, 10, 9, 12, 11)


def roll(value, shift, axis=1):
    return pltpu.roll(value, shift % value.shape[axis] if isinstance(shift, int) else shift, axis)


def collide(f, mark):
    plus = [f[i] + f[o] for i, o in PAIRS]
    minus = [f[i] - f[o] for i, o in PAIRS]
    density = f[0] + ((plus[0] + plus[1]) + (plus[2] + plus[3])) + (
        (plus[4] + plus[5]) + (plus[6] + plus[7]) + plus[8]
    )
    mx = (minus[0] + minus[3]) + (minus[4] + minus[5]) + minus[6]
    my = (minus[1] + minus[3]) - (minus[4] - minus[7]) + minus[8]
    mz = (minus[2] + minus[5]) - (minus[6] - minus[7]) - minus[8]
    inverse = 1.0 / density
    base = density - 1.5 * (mx * mx + my * my + mz * mz) * inverse
    squared = 4.5 * inverse
    along = (mx, my, mz, mx + my, mx - my, mx + mz, mx - mz, my + mz, my - mz)
    post = [None] * 19
    post[0] = f[0] - 1.25 * (f[0] - (1.0 / 3.0) * base)
    for k, (i, o) in enumerate(PAIRS):
        weight = 1.0 / 18.0 if k < 3 else 1.0 / 36.0
        m = along[k]
        even = 0.625 * plus[k] - (1.25 * weight) * (base + squared * (m * m))
        odd = (4.0 / 9.0) * minus[k] - (8.0 / 3.0 * weight) * m
        post[i] = f[i] - even - odd
        post[o] = f[o] - even + odd
    return [jnp.where(mark, f[i], post[i]) for i in range(19)], density


def group_swap(values):
    lane = lax.broadcasted_iota(jnp.int32, values[0].shape, 1)
    for bit in range(3):
        step = 1 << bit
        high = (lane // (16 * step)) % 2 == 1
        out = list(values)
        for i in range(8):
            if i & step:
                continue
            low_one, high_one = values[i], values[i + step]
            out[i] = jnp.where(high, roll(high_one, 16 * step), low_one)
            out[i + step] = jnp.where(high, high_one, roll(low_one, -16 * step))
        values = out
    return values


def kernel(pos_in, pop_in, mark_in, out, held, marks_in, held_marks, pos, send, recv, stage, ext1, ext2,
           rho, walls, rotors, face_x, face_y, face_z, edge_xy, edge_yz, edge_xz,
           got_x, got_y, got_z, got_xy, got_yz, got_xz, zext,
           in_sem, move_send, move_recv, x_send, x_recv, pair_send, pair_recv):
    s = lax.axis_index("stream")
    cy = lax.axis_index("cy")
    core = lax.axis_index("cz")
    n_s = lax.axis_size("stream")
    n_y = lax.axis_size("cy")
    up_s, down_s = lax.rem(s + 1, n_s), lax.rem(s + n_s - 1, n_s)
    up_y, down_y = lax.rem(cy + 1, n_y), lax.rem(cy + n_y - 1, n_y)
    other = 1 - core
    partners = (
        (up_s, cy, core), (down_s, cy, core), (s, up_y, core), (s, down_y, core), (s, cy, other),
        (up_s, up_y, core), (down_s, down_y, core), (up_s, down_y, core), (down_s, up_y, core),
        (s, up_y, other), (s, down_y, other), (up_s, cy, other), (down_s, cy, other),
    )
    above_s, below_s = s < n_s - 1, s > 0
    above_y, below_y = cy < n_y - 1, cy > 0
    exists = (
        above_s, below_s, above_y, below_y, None,
        above_s & above_y, below_s & below_y, above_s & below_y, below_s & above_y,
        above_y, below_y, above_s, below_s,
    )

    def when(condition, act):
        if condition is None:
            act()
        else:
            pl.when(condition)(act)

    loads = [pltpu.make_async_copy(pos_in, pos, in_sem.at[0]),
             pltpu.make_async_copy(mark_in, marks_in, in_sem.at[1])]
    loads += [
        pltpu.make_async_copy(pop_in.at[pl.ds(3 * i, 3)], held.at[pl.ds(3 * i, 3)], in_sem.at[2 + i])
        for i in range(4)
    ]
    for load in loads:
        load.start()
    barrier = pltpu.get_barrier_semaphore()
    arrivals = jnp.int32(0)
    for i, partner in enumerate(partners):
        when(exists[i], lambda partner=partner: pl.semaphore_signal(
            barrier, inc=1, device_id=partner, device_id_type=MESH))
        arrivals = arrivals + (1 if exists[i] is None else jnp.where(exists[i], 1, 0))

    loads[0].wait()
    source = [jnp.int32(-1)] * 8
    up_row = [jnp.int32(0), jnp.int32(0)]
    down_row = [jnp.int32(0), jnp.int32(0)]
    up_low, up_high = jnp.int32(99), jnp.int32(-1)
    down_low, down_high = jnp.int32(99), jnp.int32(-1)
    for r in range(ROWS):
        bx = pos[0, r]
        layer = bx - 2 * s
        bz = pos[2, r] - 4 * core
        spot = jnp.where((layer >= 0) & (layer < 2) & (bx >= 0), layer * 4 + bz, -1)
        source = [jnp.where(spot == j, r, source[j]) for j in range(8)]
        rises = layer >= 2
        sinks = (layer < 0) & (bx >= 0)
        less, more = rises & (bz < up_low), rises & (bz > up_high)
        up_row = [jnp.where(less, r, up_row[0]), jnp.where(more, r, up_row[1])]
        up_low, up_high = jnp.where(less, bz, up_low), jnp.where(more, bz, up_high)
        less, more = sinks & (bz < down_low), sinks & (bz > down_high)
        down_row = [jnp.where(less, r, down_row[0]), jnp.where(more, r, down_row[1])]
        down_low, down_high = jnp.where(less, bz, down_low), jnp.where(more, bz, down_high)
    order = []
    for layer in range(2):
        missing = jnp.int32(0)
        for z in range(4):
            order.append(jnp.minimum(missing, 1))
            missing = missing + jnp.where(source[layer * 4 + z] < 0, 1, 0)
    here = [jnp.full((8, 128), source[j], jnp.int32) >= 0 for j in range(8)]
    here4 = [jnp.full((4, 128), source[j], jnp.int32) >= 0 for j in range(8)]
    later = [jnp.full((8, 128), order[j], jnp.int32) > 0 for j in range(8)]
    second = [jnp.full((4, 128), order[j], jnp.int32) > 0 for j in range(8)]
    source = [jnp.maximum(source[j], 0) for j in range(8)]

    for load in loads[1:]:
        load.wait()
    for r in range(ROWS):
        held_marks[r] = marks_in[r:r + 1, :].astype(F32)

    def plane_of(pair, side):
        return pair + side * (15 - 2 * pair)

    def cells(k):
        return pl.ds(pl.multiple_of(k * 128, 128), 128)

    def tail(row, k):
        return jnp.concatenate([held[row, 16:19, cells(k)], held_marks[row, :, cells(k)]], axis=0)

    def move(d, c):
        return pltpu.make_async_remote_copy(
            src_ref=send.at[d, c], dst_ref=recv.at[d, c],
            send_sem=move_send.at[d, c], recv_sem=move_recv.at[d, c],
            device_id=partners[d], device_id_type=MESH,
        )

    def pack(c):
        @pl.loop(0, TILES)
        def _(kk):
            k = 2 * plane_of(c, kk // 2) + kk % 2
            for d, rows in ((0, up_row), (1, down_row)):
                for q in range(2):
                    send[d, c, kk, 2 * q] = held[rows[q], 0:8, cells(k)]
                    send[d, c, kk, 2 * q + 1] = held[rows[q], 8:16, cells(k)]
                send[d, c, kk, 4] = jnp.concatenate(
                    [tail(rows[0], k), tail(rows[1], k)], axis=0)

    pack(0)
    pl.semaphore_wait(barrier, arrivals)
    for c in range(CHUNKS):
        if c:
            pack(c)
        for d in range(2):
            when(exists[d], lambda d=d, c=c: move(d, c).start())

    lane = lax.broadcasted_iota(jnp.int32, (8, 128), 1)
    low_half = lane < 64
    flat_lane = lane % 64
    z_edge = jnp.where(core == 0, 63, 0)
    sent_z = [jnp.where(core == 0, group[3], group[4]) for group in GROUPS] + [MARK]
    edge_shift = [lax.rem(128 + j - z_edge, 128) for j in range(6)]

    def count(step):
        return 6 if step == 0 else 5

    def remote(src, dst, sems, i):
        copy = pltpu.make_async_remote_copy(
            src_ref=src, dst_ref=dst, send_sem=sems[0], recv_sem=sems[1],
            device_id=partners[i], device_id_type=MESH,
        )
        return copy, exists[i], exists[REVERSE[i]]

    def x_messages(step):
        refs = [(face_x.at[step, d], got_x.at[step, d], d) for d in range(2)]
        refs += [(edge_xy.at[step, e], got_xy.at[step, e], 5 + e) for e in range(4)]
        refs += [(edge_xz.at[step, e], got_xz.at[step, e], 11 + e) for e in range(2)]
        return [
            remote(src, dst, (x_send.at[step, k], x_recv.at[step, k]), i)
            for k, (src, dst, i) in enumerate(refs)
        ]

    def pair_messages(step, c):
        refs = [(face_y.at[step, c, d], got_y.at[step, c, d], 2 + d) for d in range(2)]
        refs += [(edge_yz.at[step, c, d], got_yz.at[step, c, d], 9 + d) for d in range(2)]
        refs += [(face_z.at[step, c], got_z.at[step, c], 4)]
        return [
            remote(src, dst, (pair_send.at[step, c, k], pair_recv.at[step, c, k]), i)
            for k, (src, dst, i) in enumerate(refs)
        ]

    def start(copies):
        for copy, there, _ in copies:
            when(there, copy.start)

    def arrive(copies):
        for copy, _, there in copies:
            when(there, copy.wait_recv)

    def outside_or(condition, value):
        return jnp.where(condition, jnp.full_like(value, 2.0), value)

    def pack_plane(ext, step, c, side, a):
        n = count(step)
        for d, pops in ((0, UP_Y), (1, DOWN_Y)):
            row = 23 if d == 0 else 8
            for j, p in enumerate((pops + (MARK,))[:n]):
                face_y[step, c, d, side, j:j + 1, :] = ext[p, a + 1, row:row + 1, :]
        for h in range(2):
            column = jnp.zeros((8, 128), F32)
            for j in range(n):
                value = ext[sent_z[j], a + 1, 8 + 8 * h:16 + 8 * h, :]
                column = jnp.where(flat_lane == j, roll(value, edge_shift[j]), column)
            face_z[step, c, side, 8 * h:8 * h + 8, :] = column
            if h == 0:
                edge_yz[step, c, 1, side, 0:1, :] = column[0:1]
            else:
                edge_yz[step, c, 0, side, 0:1, :] = column[7:8]

    def take_pair(ext, step, c):
        n = count(step)
        arrive(pair_messages(step, c))
        for side in range(2):
            a = plane_of(c, side)
            for d, pops, row in ((0, UP_Y, 7), (1, DOWN_Y, 24)):
                outside = (cy == 0) if d == 0 else (cy == n_y - 1)
                for j, p in enumerate((pops + (MARK,))[:n]):
                    value = got_y[step, c, d, side, j:j + 1, :]
                    if p == MARK:
                        value = outside_or(outside, value)
                    ext[p, a + 1, row:row + 1, :] = value
                value = got_yz[step, c, d, side, 0:1, :]
                if step == 0:
                    value = jnp.where(flat_lane[0:1] == 5, outside_or(outside, value), value)
                zext[step, a + 1, row:row + 1, :] = value
            for h in range(2):
                zext[step, a + 1, 8 + 8 * h:16 + 8 * h, :] = got_z[
                    step, c, side, 8 * h:8 * h + 8, :]

    def send_x(ext, step):
        n = count(step)
        for d, pops in ((0, UP_X), (1, DOWN_X)):
            plane = 16 if d == 0 else 1
            beyond = low_half if d == 0 else jnp.logical_not(low_half)
            for h in range(2):
                values = [
                    ext[p, plane, 8 + 8 * h:16 + 8 * h, :] for p in (pops + (MARK,))[:n]
                ]
                for j in range(0, n, 2):
                    value = roll(values[j], 64)
                    if j + 1 < n:
                        value = jnp.where(beyond, value, values[j + 1])
                    face_x[step, d, j // 2, 8 * h:8 * h + 8, :] = value
                edge_xz[step, d, 8 * h:8 * h + 8, :] = roll(
                    face_z[step, 0, 1 - d, 8 * h:8 * h + 8, :], 64)
        for e, (plane, p, row) in enumerate(((16, 7, 23), (1, 8, 8), (16, 9, 8), (1, 10, 23))):
            edge_xy[step, e, 0:1, :] = roll(ext[p, plane, row:row + 1, :], 64)
            if step == 0:
                edge_xy[step, e, 1:2, :] = roll(ext[MARK, plane, row:row + 1, :], 64)
        start(x_messages(step))

    def take_x(ext, step):
        n = count(step)
        arrive(x_messages(step))
        for d, pops in ((0, UP_X), (1, DOWN_X)):
            plane, behind = (0, 16) if d == 0 else (17, 1)
            beyond = low_half if d == 0 else jnp.logical_not(low_half)
            outside = (s == 0) if d == 0 else (s == n_s - 1)
            for h in range(2):
                rows = slice(8 + 8 * h, 16 + 8 * h)
                for j, p in enumerate((pops + (MARK,))[:n]):
                    value = got_x[step, d, j // 2, 8 * h:8 * h + 8, :]
                    if j % 2:
                        value = roll(value, 64)
                    if p == MARK:
                        value = outside_or(outside, value)
                    ext[p, plane, rows, :] = jnp.where(beyond, value, roll(ext[p, behind, rows, :], 64))
                value = got_xz[step, d, 8 * h:8 * h + 8, :]
                if step == 0:
                    value = jnp.where(flat_lane == 5, outside_or(outside, value), value)
                zext[step, plane, rows, :] = jnp.where(
                    beyond, value, roll(zext[step, behind, rows, :], 64))
        for e, (d, p, row) in enumerate(((0, 7, 7), (1, 8, 24), (0, 9, 24), (1, 10, 7))):
            plane, behind = (0, 16) if d == 0 else (17, 1)
            beyond = (low_half if d == 0 else jnp.logical_not(low_half))[0:1]
            own = roll(ext[p, behind, row:row + 1, :], 64)
            ext[p, plane, row:row + 1, :] = jnp.where(beyond, got_xy[step, e, 0:1, :], own)
            if step == 0:
                out_x = (s == 0) if d == 0 else (s == n_s - 1)
                out_y = (cy == 0) if row == 7 else (cy == n_y - 1)
                value = outside_or(out_x | out_y, got_xy[step, e, 1:2, :])
                own = roll(ext[MARK, behind, row:row + 1, :], 64)
                ext[MARK, plane, row:row + 1, :] = jnp.where(beyond, value, own)

    def settle(c):
        for d in range(2):
            when(exists[1 - d], lambda d=d: move(d, c).wait_recv())

        @pl.loop(0, 2)
        def _(side):
            a = plane_of(c, side)
            for h in range(2):
                kk = side * 2 + h
                k = 2 * a + h
                for t in range(3):
                    tiles = []
                    for j in range(8):
                        d = j // 4
                        if t < 2:
                            mine = held[source[j], 8 * t:8 * t + 8, cells(k)]
                            theirs = jnp.where(later[j], recv[d, c, kk, 2 + t], recv[d, c, kk, t])
                            tiles.append(jnp.where(here[j], mine, theirs))
                        else:
                            theirs = recv[d, c, kk, 4]
                            theirs = jnp.where(second[j], theirs[4:8], theirs[0:4])
                            tiles.append(jnp.where(here4[j], tail(source[j], k), theirs))
                    height = tiles[0].shape[0]
                    for g, value in enumerate(group_swap(tiles)):
                        stage[t, 8 * g:8 * g + height, :] = value
                f = [stage[p // 8, pl.ds(p % 8, 8, stride=8), :] for p in range(19)]
                marks = stage[2, pl.ds(3, 8, stride=8), :]
                post, density = collide(f, marks > 0.5)
                for p in range(19):
                    ext1[p, a + 1, 8 + 8 * h:16 + 8 * h, :] = post[p]
                ext1[MARK, a + 1, 8 + 8 * h:16 + 8 * h, :] = marks
                rho[a, 8 * h:8 * h + 8, :] = density
            pack_plane(ext1, 0, c, side, a)

        start(pair_messages(0, c))
        pl.when(c == 0)(lambda: send_x(ext1, 0))

    first_z = flat_lane == 0
    last_z = flat_lane == 63
    z_target = jnp.where(core == 1, 0, 63)

    def rows(h, step_y):
        start_row = 8 + 8 * h - step_y
        return slice(start_row, start_row + 8)

    halo_shift = [lax.rem(128 + z_target - j, 128) for j in range(6)]

    def z_halo(step, j, a, h, step_x, step_y):
        return roll(zext[step, a + 1 - step_x, rows(h, step_y), :], halo_shift[j])

    def make_bits(a, h):
        wall = jnp.zeros((8, 128), jnp.int32)
        rotor = jnp.zeros((8, 128), jnp.int32)

        def add(bit, value):
            nonlocal wall, rotor
            wall = wall + jnp.where(value > 0.5, 1 << bit, 0)
            if bit > 2:
                rotor = rotor + jnp.where(value == 1.0, 1 << bit, 0)

        for step_x, step_y, p_flat, p_up, p_down in GROUPS:
            value = ext1[MARK, a + 1 - step_x, rows(h, step_y), :]
            add(p_flat, value)
            halo = z_halo(0, 5, a, h, step_x, step_y)
            add(p_up, jnp.where(first_z, outside_or(core == 0, halo), roll(value, 1)))
            add(p_down, jnp.where(last_z, outside_or(core == 1, halo), roll(value, -1)))
        for step_x, step_y, p in DIAGONALS:
            add(p, ext1[MARK, a + 1 - step_x, rows(h, step_y), :])
        walls[a, 8 * h:8 * h + 8, :] = wall
        rotors[a, 8 * h:8 * h + 8, :] = rotor
        return wall, rotor

    along_z = (core * 64 + flat_lane).astype(F32) - 63.5
    drift_a = (-OMEGA / 6.0) * along_z
    sub = lax.broadcasted_iota(jnp.int32, (8, 128), 0)

    def pull(ext, step, a, h, wall, rotor):
        here_rows = slice(8 + 8 * h, 16 + 8 * h)
        centre = [ext[p, a + 1, here_rows, :] for p in range(19)]
        density = rho[a, 8 * h:8 * h + 8, :]
        along_y = (cy * 16 + 8 * h + sub).astype(F32) - 31.5
        push_a = density * drift_a
        push_b = density * ((OMEGA / 6.0) * along_y)
        both, apart = push_a + push_b, push_a - push_b
        push = {
            3: 2.0 * push_a, 4: -2.0 * push_a, 5: 2.0 * push_b, 6: -2.0 * push_b,
            7: push_a, 8: -push_a, 9: -push_a, 10: push_a,
            11: push_b, 12: -push_b, 13: -push_b, 14: push_b,
            15: both, 16: -both, 17: apart, 18: -apart,
        }
        solid = (wall & 1) != 0
        new = [None] * 19
        new[0] = centre[0]

        def settle_one(p, pulled):
            bounced = centre[OPPOSITE[p]]
            if p > 2:
                bounced = bounced + jnp.where((rotor & (1 << p)) != 0, push[p], 0.0)
            value = jnp.where((wall & (1 << p)) != 0, bounced, pulled)
            new[p] = jnp.where(solid, centre[p], value)

        for j, (step_x, step_y, p_flat, p_up, p_down) in enumerate(GROUPS):
            if p_flat:
                settle_one(p_flat, ext[p_flat, a + 1 - step_x, rows(h, step_y), :])
            halo = z_halo(step, j, a, h, step_x, step_y)
            value = ext[p_up, a + 1 - step_x, rows(h, step_y), :]
            settle_one(p_up, jnp.where(first_z, halo, roll(value, 1)))
            value = ext[p_down, a + 1 - step_x, rows(h, step_y), :]
            settle_one(p_down, jnp.where(last_z, halo, roll(value, -1)))
        for step_x, step_y, p in DIAGONALS:
            settle_one(p, ext[p, a + 1 - step_x, rows(h, step_y), :])
        return new, solid

    def middle(p):
        def taken(p):
            return jnp.where(p < 0, 0, jnp.where(p < 4, p + 3, jnp.minimum(p + 2, 8)))

        @pl.loop(taken(p - 1), taken(p))
        def _(c):
            take_pair(ext1, 0, c)

        pl.when(p == 4)(lambda: take_x(ext1, 0))
        c = jnp.where(p < 4, p + 1, jnp.where(p == 4, 0, p))

        @pl.loop(0, 2)
        def _(side):
            a = plane_of(c, side)
            for h in range(2):
                wall, rotor = make_bits(a, h)
                new, solid = pull(ext1, 0, a, h, wall, rotor)
                post, density = collide(new, solid)
                for p in range(19):
                    ext2[p, a + 1, 8 + 8 * h:16 + 8 * h, :] = post[p]
                rho[a, 8 * h:8 * h + 8, :] = density
            pack_plane(ext2, 1, c, side, a)

        start(pair_messages(1, c))
        pl.when(p == 4)(lambda: send_x(ext2, 1))

    def last(p):
        def taken(p):
            return jnp.where(p < 0, 0, jnp.minimum(p + 3, 8))

        @pl.loop(taken(p - 1), taken(p))
        def _(u):
            take_pair(ext2, 1, jnp.where(u < 5, u + 1, jnp.where(u == 5, 0, u)))

        pl.when(p == 7)(lambda: take_x(ext2, 1))
        c = jnp.where(p < 3, p + 2, jnp.where(p == 3, 1, jnp.where(p == 7, 0, p + 1)))

        @pl.loop(0, 2)
        def _(side):
            a = plane_of(c, side)
            for h in range(2):
                wall = walls[a, 8 * h:8 * h + 8, :]
                rotor = rotors[a, 8 * h:8 * h + 8, :]
                new, _ = pull(ext2, 1, a, h, wall, rotor)
                for p in range(19):
                    out[p, a, 8 * h:8 * h + 8, :] = new[p][:, 0:64]
                    out[p, EDGE + a, 8 * h:8 * h + 8, :] = roll(new[p], 64)[:, 0:64]

    def collided(t):
        return jnp.where(t >= 9, 8, jnp.where(t == 8, 6, jnp.clip(t - 3, 0, 4)))

    def streamed(t):
        return jnp.where(t >= 10, 8, jnp.where(t == 9, 1, 0))

    def tick(t, carry):
        @pl.loop(streamed(t - 1), streamed(t))
        def _(c):
            last(c)

        pl.when(t < CHUNKS)(lambda: settle(t))

        @pl.loop(collided(t - 1), collided(t))
        def _(c):
            middle(c)

        return carry

    lax.fori_loop(0, 11, tick, 0)
    for c in range(CHUNKS):
        for d in range(2):
            when(exists[d], lambda d=d, c=c: move(d, c).wait_send())
    for step in range(2):
        for copy, there, _ in x_messages(step):
            when(there, copy.wait_send)
        for c in range(CHUNKS):
            for copy, there, _ in pair_messages(step, c):
                when(there, copy.wait_send)


def step_all(populations, solid_cells, block_pos):
    scratch = [
        pltpu.VMEM((ROWS, 19, 4096), F32),
        pltpu.VMEM((ROWS, 4096), jnp.int32),
        pltpu.VMEM((ROWS, 1, 4096), F32),
        pltpu.SMEM((3, ROWS), jnp.int32),
        pltpu.VMEM((2, CHUNKS, TILES, 5, 8, 128), F32),
        pltpu.VMEM((2, CHUNKS, TILES, 5, 8, 128), F32),
        pltpu.VMEM((3, 64, 128), F32),
        pltpu.VMEM((20, 18, 32, 128), F32),
        pltpu.VMEM((20, 18, 32, 128), F32),
        pltpu.VMEM((EDGE, 16, 128), F32),
        pltpu.VMEM((EDGE, 16, 128), jnp.int32),
        pltpu.VMEM((EDGE, 16, 128), jnp.int32),
    ]
    for _ in range(2):
        scratch += [
            pltpu.VMEM((2, 2, 3, 16, 128), F32),
            pltpu.VMEM((2, CHUNKS, 2, 2, 8, 128), F32),
            pltpu.VMEM((2, CHUNKS, 2, 16, 128), F32),
            pltpu.VMEM((2, 4, 8, 128), F32),
            pltpu.VMEM((2, CHUNKS, 2, 2, 8, 128), F32),
            pltpu.VMEM((2, 2, 16, 128), F32),
        ]
    scratch += [
        pltpu.VMEM((2, 18, 32, 128), F32),
        pltpu.SemaphoreType.DMA((6,)),
        pltpu.SemaphoreType.DMA((2, CHUNKS)),
        pltpu.SemaphoreType.DMA((2, CHUNKS)),
        pltpu.SemaphoreType.DMA((2, 8)),
        pltpu.SemaphoreType.DMA((2, 8)),
        pltpu.SemaphoreType.DMA((2, CHUNKS, 5)),
        pltpu.SemaphoreType.DMA((2, CHUNKS, 5)),
    ]
    return pl.pallas_call(
        kernel,
        out_shape=jax.ShapeDtypeStruct((19, 32, 16, 64), F32),
        in_specs=[pl.BlockSpec(memory_space=pltpu.HBM)] * 3,
        out_specs=pl.BlockSpec(memory_space=pltpu.VMEM),
        scratch_shapes=scratch,
        compiler_params=pltpu.CompilerParams(
            collective_id=0, has_side_effects=True, vmem_limit_bytes=40 * 1024 * 1024
        ),
    )(*(pltpu.with_memory_space_constraint(value, pltpu.HBM)
        for value in (block_pos.T, populations, solid_cells)))


def solution(mesh):
    in_specs = (
        P(("stream", "cy", "cz"), None, None),
        P(("stream", "cy", "cz"), None),
        P(("stream", "cy", "cz"), None),
    )
    out_specs = P(None, "stream", "cy", "cz")
    return jax.shard_map(step_all, mesh=mesh, in_specs=in_specs, out_specs=out_specs, check_vma=False)
```

```python
import jax
import jax.numpy as jnp
from jax import lax
from jax.experimental import pallas as pl
from jax.experimental.pallas import tpu as pltpu
from jax.sharding import PartitionSpec as P

MESH = pl.DeviceIdType.MESH
F32 = jnp.float32

GROUPS = (
    (0, 0, 0, 5, 6),
    (1, 0, 1, 11, 13),
    (-1, 0, 2, 14, 12),
    (0, 1, 3, 15, 17),
    (0, -1, 4, 18, 16),
)
DIAGONALS = ((1, 1, 7), (-1, -1, 8), (1, -1, 9), (-1, 1, 10))
PAIRS = ((1, 2), (3, 4), (5, 6), (7, 8), (9, 10), (11, 12), (13, 14), (15, 16), (17, 18))
OPPOSITE = (0, 2, 1, 4, 3, 6, 5, 8, 7, 10, 9, 12, 11, 14, 13, 16, 15, 18, 17)
UP_X = (1, 7, 9, 11, 13)
DOWN_X = (2, 8, 10, 12, 14)
UP_Y = (3, 7, 10, 15, 17)
DOWN_Y = (4, 8, 9, 16, 18)
MARK = 19
ROTOR_CODE = 0x10001

EDGE = 16
CHUNKS = 8
TILES = 4
ROWS = 12
OMEGA = 0.2 / 192.0
REVERSE = (1, 0, 3, 2, 4, 6, 5, 8, 7, 10, 9, 12, 11)


def roll(value, shift, axis=1):
    return pltpu.roll(value, shift % value.shape[axis] if isinstance(shift, int) else shift, axis)


def collide(f, mark):
    plus = [f[i] + f[o] for i, o in PAIRS]
    minus = [f[i] - f[o] for i, o in PAIRS]
    density = f[0] + ((plus[0] + plus[1]) + (plus[2] + plus[3])) + (
        (plus[4] + plus[5]) + (plus[6] + plus[7]) + plus[8]
    )
    mx = (minus[0] + minus[3]) + (minus[4] + minus[5]) + minus[6]
    my = (minus[1] + minus[3]) - (minus[4] - minus[7]) + minus[8]
    mz = (minus[2] + minus[5]) - (minus[6] - minus[7]) - minus[8]
    inverse = 1.0 / density
    base = density - 1.5 * (mx * mx + my * my + mz * mz) * inverse
    squared = 4.5 * inverse
    along = (mx, my, mz, mx + my, mx - my, mx + mz, mx - mz, my + mz, my - mz)
    post = [None] * 19
    post[0] = f[0] - 1.25 * (f[0] - (1.0 / 3.0) * base)
    for k, (i, o) in enumerate(PAIRS):
        weight = 1.0 / 18.0 if k < 3 else 1.0 / 36.0
        m = along[k]
        even = 0.625 * plus[k] - (1.25 * weight) * (base + squared * (m * m))
        odd = (4.0 / 9.0) * minus[k] - (8.0 / 3.0 * weight) * m
        post[i] = f[i] - even - odd
        post[o] = f[o] - even + odd
    return [jnp.where(mark, f[0], post[0])] + [jnp.where(mark, f[OPPOSITE[i]], post[i]) for i in range(1, 19)], density


def group_swap(values):
    lane = lax.broadcasted_iota(jnp.int32, values[0].shape, 1)
    for bit in range(3):
        step = 1 << bit
        high = (lane // (16 * step)) % 2 == 1
        out = list(values)
        for i in range(8):
            if i & step:
                continue
            low_one, high_one = values[i], values[i + step]
            out[i] = jnp.where(high, roll(high_one, 16 * step), low_one)
            out[i + step] = jnp.where(high, high_one, roll(low_one, -16 * step))
        values = out
    return values


def kernel(pos_in, pop_in, mark_in, out, held, marks_in, held_marks, pos, send, recv, stage, ext1, ext2,
           codes, rho, walls, rotors, face_x, face_y, face_z, edge_xy, edge_yz, edge_xz,
           got_x, got_y, got_z, got_xy, got_yz, got_xz, zext,
           in_sem, move_send, move_recv, x_send, x_recv, pair_send, pair_recv):
    s = lax.axis_index("stream")
    cy = lax.axis_index("cy")
    core = lax.axis_index("cz")
    n_s = lax.axis_size("stream")
    n_y = lax.axis_size("cy")
    up_s, down_s = lax.rem(s + 1, n_s), lax.rem(s + n_s - 1, n_s)
    up_y, down_y = lax.rem(cy + 1, n_y), lax.rem(cy + n_y - 1, n_y)
    other = 1 - core
    partners = (
        (up_s, cy, core), (down_s, cy, core), (s, up_y, core), (s, down_y, core), (s, cy, other),
        (up_s, up_y, core), (down_s, down_y, core), (up_s, down_y, core), (down_s, up_y, core),
        (s, up_y, other), (s, down_y, other), (up_s, cy, other), (down_s, cy, other),
    )
    above_s, below_s = s < n_s - 1, s > 0
    above_y, below_y = cy < n_y - 1, cy > 0
    exists = (
        above_s, below_s, above_y, below_y, None,
        above_s & above_y, below_s & below_y, above_s & below_y, below_s & above_y,
        above_y, below_y, above_s, below_s,
    )

    def when(condition, act):
        if condition is None:
            act()
        else:
            pl.when(condition)(act)

    loads = [pltpu.make_async_copy(pos_in, pos, in_sem.at[0]),
             pltpu.make_async_copy(mark_in, marks_in, in_sem.at[1])]
    loads += [
        pltpu.make_async_copy(
            pop_in.at[pl.ds(3 * i, 3)], held.at[pl.ds(3 * i, 3), :, pl.ds(0, 4096)], in_sem.at[2 + i])
        for i in range(4)
    ]
    for load in loads:
        load.start()
    barrier = pltpu.get_barrier_semaphore()
    arrivals = jnp.int32(0)
    for i, partner in enumerate(partners):
        when(exists[i], lambda partner=partner: pl.semaphore_signal(
            barrier, inc=1, device_id=partner, device_id_type=MESH))
        arrivals = arrivals + (1 if exists[i] is None else jnp.where(exists[i], 1, 0))

    loads[0].wait()
    source = [jnp.int32(-1)] * 8
    up_row = [jnp.int32(0), jnp.int32(0)]
    down_row = [jnp.int32(0), jnp.int32(0)]
    up_low, up_high = jnp.int32(99), jnp.int32(-1)
    down_low, down_high = jnp.int32(99), jnp.int32(-1)
    for r in range(ROWS):
        bx = pos[0, r]
        layer = bx - 2 * s
        bz = pos[2, r] - 4 * core
        spot = jnp.where((layer >= 0) & (layer < 2) & (bx >= 0), layer * 4 + bz, -1)
        source = [jnp.where(spot == j, r, source[j]) for j in range(8)]
        rises = layer >= 2
        sinks = (layer < 0) & (bx >= 0)
        less, more = rises & (bz < up_low), rises & (bz > up_high)
        up_row = [jnp.where(less, r, up_row[0]), jnp.where(more, r, up_row[1])]
        up_low, up_high = jnp.where(less, bz, up_low), jnp.where(more, bz, up_high)
        less, more = sinks & (bz < down_low), sinks & (bz > down_high)
        down_row = [jnp.where(less, r, down_row[0]), jnp.where(more, r, down_row[1])]
        down_low, down_high = jnp.where(less, bz, down_low), jnp.where(more, bz, down_high)
    order = []
    for layer in range(2):
        missing = jnp.int32(0)
        for z in range(4):
            order.append(jnp.minimum(missing, 1))
            missing = missing + jnp.where(source[layer * 4 + z] < 0, 1, 0)
    source = [
        jnp.where(source[j] < 0, ROWS + 2 * (j // 4) + order[j], source[j]) for j in range(8)
    ]

    for load in loads[1:]:
        load.wait()
    for r in range(ROWS):
        held_marks[r] = marks_in[r:r + 1, :].astype(F32)

    def plane_of(pair, side):
        return pair + side * (15 - 2 * pair)

    def cells(k):
        return pl.ds(pl.multiple_of(k * 128, 128), 128)

    def tail(row, k):
        return jnp.concatenate([held[row, 16:19, cells(k)], held_marks[row, :, cells(k)]], axis=0)

    def move(d, c):
        return pltpu.make_async_remote_copy(
            src_ref=send.at[d, c], dst_ref=recv.at[d, c],
            send_sem=move_send.at[d, c], recv_sem=move_recv.at[d, c],
            device_id=partners[d], device_id_type=MESH,
        )

    def pack(c):
        @pl.loop(0, TILES)
        def _(kk):
            k = 2 * plane_of(c, kk // 2) + kk % 2
            for d, rows in ((0, up_row), (1, down_row)):
                for q in range(2):
                    send[d, c, kk, 2 * q] = held[rows[q], 0:8, cells(k)]
                    send[d, c, kk, 2 * q + 1] = held[rows[q], 8:16, cells(k)]
                send[d, c, kk, 4] = jnp.concatenate(
                    [tail(rows[0], k), tail(rows[1], k)], axis=0)

    pack(0)
    pl.semaphore_wait(barrier, arrivals)
    for c in range(CHUNKS):
        if c:
            pack(c)
        for d in range(2):
            when(exists[d], lambda d=d, c=c: move(d, c).start())

    lane = lax.broadcasted_iota(jnp.int32, (8, 128), 1)
    low_half = lane < 64
    flat_lane = lane % 64
    z_edge = jnp.where(core == 0, 63, 0)
    sent_z = [jnp.where(core == 0, group[3], group[4]) for group in GROUPS] + [MARK]
    edge_shift = [lax.rem(128 + j - z_edge, 128) for j in range(6)]

    def count(step):
        return 6 if step == 0 else 5

    def remote(src, dst, sems, i):
        copy = pltpu.make_async_remote_copy(
            src_ref=src, dst_ref=dst, send_sem=sems[0], recv_sem=sems[1],
            device_id=partners[i], device_id_type=MESH,
        )
        return copy, exists[i], exists[REVERSE[i]]

    def x_messages(step):
        refs = [(face_x.at[step, d], got_x.at[step, d], d) for d in range(2)]
        refs += [(edge_xy.at[step, e], got_xy.at[step, e], 5 + e) for e in range(4)]
        refs += [(edge_xz.at[step, e], got_xz.at[step, e], 11 + e) for e in range(2)]
        return [
            remote(src, dst, (x_send.at[step, k], x_recv.at[step, k]), i)
            for k, (src, dst, i) in enumerate(refs)
        ]

    def pair_messages(step, c):
        refs = [(face_y.at[step, c, d], got_y.at[step, c, d], 2 + d) for d in range(2)]
        refs += [(edge_yz.at[step, c, d], got_yz.at[step, c, d], 9 + d) for d in range(2)]
        refs += [(face_z.at[step, c], got_z.at[step, c], 4)]
        return [
            remote(src, dst, (pair_send.at[step, c, k], pair_recv.at[step, c, k]), i)
            for k, (src, dst, i) in enumerate(refs)
        ]

    def start(copies):
        for copy, there, _ in copies:
            when(there, copy.start)

    def arrive(copies):
        for copy, _, there in copies:
            when(there, copy.wait_recv)

    def outside_or(condition, value):
        return jnp.where(condition, jnp.full_like(value, 2.0), value)

    def code_or(condition, value):
        code = jnp.where(value > 0.5, ROTOR_CODE, 0)
        return jnp.where(condition, jnp.full_like(code, 1), code)

    def pack_plane(ext, step, c, side, a):
        n = count(step)
        for d, pops in ((0, UP_Y), (1, DOWN_Y)):
            row = 23 if d == 0 else 8
            for j, p in enumerate((pops + (MARK,))[:n]):
                face_y[step, c, d, side, j:j + 1, :] = ext[p, a + 1, row:row + 1, :]
        for h in range(2):
            column = jnp.zeros((8, 128), F32)
            for j in range(n):
                value = ext[sent_z[j], a + 1, 8 + 8 * h:16 + 8 * h, :]
                column = jnp.where(flat_lane == j, roll(value, edge_shift[j]), column)
            face_z[step, c, side, 8 * h:8 * h + 8, :] = column
            if h == 0:
                edge_yz[step, c, 1, side, 0:1, :] = column[0:1]
            else:
                edge_yz[step, c, 0, side, 0:1, :] = column[7:8]

    def take_pair(ext, step, c):
        n = count(step)
        arrive(pair_messages(step, c))
        for side in range(2):
            a = plane_of(c, side)
            for d, pops, row in ((0, UP_Y, 7), (1, DOWN_Y, 24)):
                outside = (cy == 0) if d == 0 else (cy == n_y - 1)
                for j, p in enumerate((pops + (MARK,))[:n]):
                    value = got_y[step, c, d, side, j:j + 1, :]
                    if p == MARK:
                        codes[a + 1, row:row + 1, :] = code_or(outside, value)
                    else:
                        ext[p, a + 1, row:row + 1, :] = value
                value = got_yz[step, c, d, side, 0:1, :]
                if step == 0:
                    value = jnp.where(flat_lane[0:1] == 5, outside_or(outside, value), value)
                zext[step, a + 1, row:row + 1, :] = value
            for h in range(2):
                zext[step, a + 1, 8 + 8 * h:16 + 8 * h, :] = got_z[
                    step, c, side, 8 * h:8 * h + 8, :]

    def send_x(ext, step):
        n = count(step)
        for d, pops in ((0, UP_X), (1, DOWN_X)):
            plane = 16 if d == 0 else 1
            beyond = low_half if d == 0 else jnp.logical_not(low_half)
            for h in range(2):
                values = [
                    ext[p, plane, 8 + 8 * h:16 + 8 * h, :] for p in (pops + (MARK,))[:n]
                ]
                for j in range(0, n, 2):
                    value = roll(values[j], 64)
                    if j + 1 < n:
                        value = jnp.where(beyond, value, values[j + 1])
                    face_x[step, d, j // 2, 8 * h:8 * h + 8, :] = value
                edge_xz[step, d, 8 * h:8 * h + 8, :] = roll(
                    face_z[step, 0, 1 - d, 8 * h:8 * h + 8, :], 64)
        for e, (plane, p, row) in enumerate(((16, 7, 23), (1, 8, 8), (16, 9, 8), (1, 10, 23))):
            edge_xy[step, e, 0:1, :] = roll(ext[p, plane, row:row + 1, :], 64)
            if step == 0:
                edge_xy[step, e, 1:2, :] = roll(ext[MARK, plane, row:row + 1, :], 64)
        start(x_messages(step))

    def take_x(ext, step):
        n = count(step)
        arrive(x_messages(step))
        for d, pops in ((0, UP_X), (1, DOWN_X)):
            plane, behind = (0, 16) if d == 0 else (17, 1)
            beyond = low_half if d == 0 else jnp.logical_not(low_half)
            outside = (s == 0) if d == 0 else (s == n_s - 1)
            for h in range(2):
                rows = slice(8 + 8 * h, 16 + 8 * h)
                for j, p in enumerate((pops + (MARK,))[:n]):
                    value = got_x[step, d, j // 2, 8 * h:8 * h + 8, :]
                    if j % 2:
                        value = roll(value, 64)
                    if p == MARK:
                        codes[plane, rows, :] = jnp.where(
                            beyond, code_or(outside, value), roll(codes[behind, rows, :], 64))
                    else:
                        ext[p, plane, rows, :] = jnp.where(
                            beyond, value, roll(ext[p, behind, rows, :], 64))
                value = got_xz[step, d, 8 * h:8 * h + 8, :]
                if step == 0:
                    value = jnp.where(flat_lane == 5, outside_or(outside, value), value)
                zext[step, plane, rows, :] = jnp.where(
                    beyond, value, roll(zext[step, behind, rows, :], 64))
        for e, (d, p, row) in enumerate(((0, 7, 7), (1, 8, 24), (0, 9, 24), (1, 10, 7))):
            plane, behind = (0, 16) if d == 0 else (17, 1)
            beyond = (low_half if d == 0 else jnp.logical_not(low_half))[0:1]
            own = roll(ext[p, behind, row:row + 1, :], 64)
            ext[p, plane, row:row + 1, :] = jnp.where(beyond, got_xy[step, e, 0:1, :], own)
            if step == 0:
                out_x = (s == 0) if d == 0 else (s == n_s - 1)
                out_y = (cy == 0) if row == 7 else (cy == n_y - 1)
                value = code_or(out_x | out_y, got_xy[step, e, 1:2, :])
                own = roll(codes[behind, row:row + 1, :], 64)
                codes[plane, row:row + 1, :] = jnp.where(beyond, value, own)

    def settle(c):
        for d in range(2):
            when(exists[1 - d], lambda d=d: move(d, c).wait_recv())

        @pl.loop(0, TILES)
        def _(kk):
            k = 2 * plane_of(c, kk // 2) + kk % 2
            for d in range(2):
                last_rows = recv[d, c, kk, 4]
                for q in range(2):
                    row = ROWS + 2 * d + q
                    held[row, 0:8, cells(k)] = recv[d, c, kk, 2 * q]
                    held[row, 8:16, cells(k)] = recv[d, c, kk, 2 * q + 1]
                    held[row, 16:19, cells(k)] = last_rows[4 * q:4 * q + 3]
                    held_marks[row, :, cells(k)] = last_rows[4 * q + 3:4 * q + 4]

        @pl.loop(0, 2)
        def _(side):
            a = plane_of(c, side)
            for h in range(2):
                k = 2 * a + h
                for t in range(3):
                    if t < 2:
                        tiles = [held[source[j], 8 * t:8 * t + 8, cells(k)] for j in range(8)]
                    else:
                        tiles = [tail(source[j], k) for j in range(8)]
                    height = tiles[0].shape[0]
                    for g, value in enumerate(group_swap(tiles)):
                        stage[h, t, 9 * g:9 * g + height, :] = value
            for h in range(2):
                f = [stage[h, p // 8, pl.ds(p % 8, 8, stride=9), :] for p in range(19)]
                marks = stage[h, 2, pl.ds(3, 8, stride=9), :]
                post, density = collide(f, marks > 0.5)
                for p in range(19):
                    ext1[p, a + 1, 8 + 8 * h:16 + 8 * h, :] = post[p]
                ext1[MARK, a + 1, 8 + 8 * h:16 + 8 * h, :] = marks
                codes[a + 1, 8 + 8 * h:16 + 8 * h, :] = jnp.where(marks > 0.5, ROTOR_CODE, 0)
                rho[a, 8 * h:8 * h + 8, :] = density
            pack_plane(ext1, 0, c, side, a)

        start(pair_messages(0, c))
        pl.when(c == 0)(lambda: send_x(ext1, 0))

    first_z = flat_lane == 0
    last_z = flat_lane == 63
    z_target = jnp.where(core == 1, 0, 63)

    def rows(h, step_y):
        start_row = 8 + 8 * h - step_y
        return slice(start_row, start_row + 8)

    halo_shift = [lax.rem(128 + z_target - j, 128) for j in range(6)]

    def z_halo(step, j, a, h, step_x, step_y):
        return roll(zext[step, a + 1 - step_x, rows(h, step_y), :], halo_shift[j])

    def make_bits(a, h):
        words = [jnp.zeros((8, 128), jnp.int32)] * 2

        def add(p, code):
            words[p // 16] = words[p // 16] | (code << (p - 15 * (p // 16)))

        solid = None
        for step_x, step_y, p_flat, p_up, p_down in GROUPS:
            code = codes[a + 1 - step_x, rows(h, step_y), :]
            if p_flat:
                add(p_flat, code)
            else:
                solid = code != 0
            halo = z_halo(0, 5, a, h, step_x, step_y)
            halo = jnp.where(halo > 1.5, 1, jnp.where(halo > 0.5, ROTOR_CODE, 0))
            wall = jnp.full_like(code, 1)
            add(p_up, jnp.where(first_z, jnp.where(core == 0, wall, halo), roll(code, 1)))
            add(p_down, jnp.where(last_z, jnp.where(core == 1, wall, halo), roll(code, -1)))
        for step_x, step_y, p in DIAGONALS:
            add(p, codes[a + 1 - step_x, rows(h, step_y), :])
        walls[a, 8 * h:8 * h + 8, :] = jnp.where(solid, 0xFFFF, words[0])
        rotors[a, 8 * h:8 * h + 8, :] = jnp.where(solid, 0xE, words[1])
        return walls[a, 8 * h:8 * h + 8, :], rotors[a, 8 * h:8 * h + 8, :]

    def bit(words, p, base):
        at = base + p - 15 * (p // 16)
        return (words[p // 16] & (-(1 << 31) if at == 31 else 1 << at)) != 0

    along_z = (core * 64 + flat_lane).astype(F32) - 63.5
    drift_a = (-OMEGA / 6.0) * along_z
    sub = lax.broadcasted_iota(jnp.int32, (8, 128), 0)

    def pull(ext, step, a, h, words):
        here_rows = slice(8 + 8 * h, 16 + 8 * h)
        centre = [ext[p, a + 1, here_rows, :] for p in range(19)]
        density = rho[a, 8 * h:8 * h + 8, :]
        along_y = (cy * 16 + 8 * h + sub).astype(F32) - 31.5
        push_a = density * drift_a
        push_b = density * ((OMEGA / 6.0) * along_y)
        both, apart = push_a + push_b, push_a - push_b
        push = {
            3: 2.0 * push_a, 4: -2.0 * push_a, 5: 2.0 * push_b, 6: -2.0 * push_b,
            7: push_a, 8: -push_a, 9: -push_a, 10: push_a,
            11: push_b, 12: -push_b, 13: -push_b, 14: push_b,
            15: both, 16: -both, 17: apart, 18: -apart,
        }
        solid = bit(words, 0, 0)
        new = [None] * 19
        new[0] = centre[0]

        def settle_one(p, pulled):
            bounced = centre[OPPOSITE[p]]
            if p > 2:
                bounced = bounced + jnp.where(bit(words, p, 16), push[p], 0.0)
            new[p] = jnp.where(bit(words, p, 0), bounced, pulled)

        for j, (step_x, step_y, p_flat, p_up, p_down) in enumerate(GROUPS):
            if p_flat:
                settle_one(p_flat, ext[p_flat, a + 1 - step_x, rows(h, step_y), :])
            halo = z_halo(step, j, a, h, step_x, step_y)
            value = ext[p_up, a + 1 - step_x, rows(h, step_y), :]
            settle_one(p_up, jnp.where(first_z, halo, roll(value, 1)))
            value = ext[p_down, a + 1 - step_x, rows(h, step_y), :]
            settle_one(p_down, jnp.where(last_z, halo, roll(value, -1)))
        for step_x, step_y, p in DIAGONALS:
            settle_one(p, ext[p, a + 1 - step_x, rows(h, step_y), :])
        return new, solid

    def middle(p):
        def taken(p):
            return jnp.where(p < 0, 0, jnp.where(p < 4, p + 3, jnp.minimum(p + 2, 8)))

        @pl.loop(taken(p - 1), taken(p))
        def _(c):
            take_pair(ext1, 0, c)

        pl.when(p == 4)(lambda: take_x(ext1, 0))
        c = jnp.where(p < 4, p + 1, jnp.where(p == 4, 0, p))

        @pl.loop(0, 2)
        def _(side):
            a = plane_of(c, side)
            for h in range(2):
                new, solid = pull(ext1, 0, a, h, make_bits(a, h))
                post, density = collide(new, solid)
                for p in range(19):
                    ext2[p, a + 1, 8 + 8 * h:16 + 8 * h, :] = post[p]
                rho[a, 8 * h:8 * h + 8, :] = density
            pack_plane(ext2, 1, c, side, a)

        start(pair_messages(1, c))
        pl.when(p == 4)(lambda: send_x(ext2, 1))

    def last(p):
        def taken(p):
            return jnp.where(p < 0, 0, jnp.minimum(p + 3, 8))

        @pl.loop(taken(p - 1), taken(p))
        def _(u):
            take_pair(ext2, 1, jnp.where(u < 5, u + 1, jnp.where(u == 5, 0, u)))

        pl.when(p == 7)(lambda: take_x(ext2, 1))
        c = jnp.where(p < 3, p + 2, jnp.where(p == 3, 1, jnp.where(p == 7, 0, p + 1)))

        @pl.loop(0, 2)
        def _(side):
            a = plane_of(c, side)
            for h in range(2):
                words = (walls[a, 8 * h:8 * h + 8, :], rotors[a, 8 * h:8 * h + 8, :])
                new, _ = pull(ext2, 1, a, h, words)
                for p in range(19):
                    out[p, a, 8 * h:8 * h + 8, :] = new[p][:, 0:64]
                    out[p, EDGE + a, 8 * h:8 * h + 8, :] = roll(new[p], 64)[:, 0:64]

    def collided(t):
        return jnp.where(t >= 9, 8, jnp.where(t == 8, 6, jnp.clip(t - 3, 0, 4)))

    def streamed(t):
        return jnp.where(t >= 10, 8, 0)

    def tick(t, carry):
        @pl.loop(streamed(t - 1), streamed(t))
        def _(c):
            last(c)

        pl.when(t < CHUNKS)(lambda: settle(t))

        @pl.loop(collided(t - 1), collided(t))
        def _(c):
            middle(c)

        return carry

    lax.fori_loop(0, 11, tick, 0)
    for c in range(CHUNKS):
        for d in range(2):
            when(exists[d], lambda d=d, c=c: move(d, c).wait_send())
    for step in range(2):
        for copy, there, _ in x_messages(step):
            when(there, copy.wait_send)
        for c in range(CHUNKS):
            for copy, there, _ in pair_messages(step, c):
                when(there, copy.wait_send)


def step_all(populations, solid_cells, block_pos):
    scratch = [
        pltpu.VMEM((ROWS + 4, 19, 4224), F32),
        pltpu.VMEM((ROWS, 4096), jnp.int32),
        pltpu.VMEM((ROWS + 5, 1, 4096), F32),
        pltpu.SMEM((3, ROWS), jnp.int32),
        pltpu.VMEM((2, CHUNKS, TILES, 5, 8, 128), F32),
        pltpu.VMEM((2, CHUNKS, TILES, 5, 8, 128), F32),
        pltpu.VMEM((2, 3, 88, 128), F32),
        pltpu.VMEM((20, 19, 40, 128), F32),
        pltpu.VMEM((20, 19, 40, 128), F32),
        pltpu.VMEM((18, 32, 128), jnp.int32),
        pltpu.VMEM((EDGE, 16, 128), F32),
        pltpu.VMEM((EDGE, 16, 128), jnp.int32),
        pltpu.VMEM((EDGE, 16, 128), jnp.int32),
    ]
    for _ in range(2):
        scratch += [
            pltpu.VMEM((2, 2, 3, 16, 128), F32),
            pltpu.VMEM((2, CHUNKS + 1, 2, 2, 8, 128), F32),
            pltpu.VMEM((2, CHUNKS, 2, 16, 128), F32),
            pltpu.VMEM((2, 4, 8, 128), F32),
            pltpu.VMEM((2, CHUNKS + 1, 2, 2, 8, 128), F32),
            pltpu.VMEM((2, 2, 16, 128), F32),
        ]
    scratch += [
        pltpu.VMEM((2, 18, 32, 128), F32),
        pltpu.SemaphoreType.DMA((6,)),
        pltpu.SemaphoreType.DMA((2, CHUNKS)),
        pltpu.SemaphoreType.DMA((2, CHUNKS)),
        pltpu.SemaphoreType.DMA((2, 8)),
        pltpu.SemaphoreType.DMA((2, 8)),
        pltpu.SemaphoreType.DMA((2, CHUNKS, 5)),
        pltpu.SemaphoreType.DMA((2, CHUNKS, 5)),
    ]
    return pl.pallas_call(
        kernel,
        out_shape=jax.ShapeDtypeStruct((19, 32, 16, 64), F32),
        in_specs=[pl.BlockSpec(memory_space=pltpu.HBM)] * 3,
        out_specs=pl.BlockSpec(memory_space=pltpu.VMEM),
        scratch_shapes=scratch,
        compiler_params=pltpu.CompilerParams(
            collective_id=0, has_side_effects=True, vmem_limit_bytes=44 * 1024 * 1024
        ),
    )(*(pltpu.with_memory_space_constraint(value, pltpu.HBM)
        for value in (block_pos.T, populations, solid_cells)))


def solution(mesh):
    in_specs = (
        P(("stream", "cy", "cz"), None, None),
        P(("stream", "cy", "cz"), None),
        P(("stream", "cy", "cz"), None),
    )
    out_specs = P(None, "stream", "cy", "cz")
    return jax.shard_map(step_all, mesh=mesh, in_specs=in_specs, out_specs=out_specs, check_vma=False)
```
